512 devices in a mesh: rep: 2 (over y), seq: 32 (over z), tp: 8 (over x, core).
Axes of the slice: x: 4, y: 2, z: 32, core: 2. Of those that a mesh axis runs over, the one named last changes fastest.
The devices are a block of a 4x8x32 slice.
Arguments:
- queries: bfloat16 [128, 64, 128], P(('rep', 'seq')), parts along dimension 0, may hold values from -9 to 9
- key_pages: bfloat16 [8192, 8, 64, 128], P(('rep', 'seq'), 'tp'), parts along dimension 0, may hold values from -4 to 4
- value_pages: bfloat16 [8192, 8, 64, 128], P(('rep', 'seq'), 'tp'), parts along dimension 0, may hold values from -6 to 6
- page_owner: int32 [128, 1024], P('rep'), parts along dimension 0, may hold values from 0 to 31, as said below
- page_local: int32 [128, 1024], P('rep'), parts along dimension 0, may hold values from 0 to 127, as said below
- seq_lengths: int32 [128], P('rep'), parts along dimension 0, may hold values from 1 to 65536, as said below
Outputs:
- attention: bfloat16 [128, 64, 128], P(('rep', 'seq'), 'tp'), parts along dimension 0
The draws below stay inside these ranges and needn't reach their ends.
There are 2 independent parts, one for each index of `rep`. The reference program is written for one: setup_inputs(seed, part) draws one part's arguments, and reference() takes and returns one part's arrays. A program takes and returns all parts, laid end to end along the dimension named above; each array names one. Nothing has to cross between parts.
Inputs may be any that keep to these rules, and one draw needn't show every extreme that they name: The live slots (s * 64 < seq_lengths[b]) name pairs (page_owner, page_local) that are all different; the other slots hold 0. `page_local`: see page_owner. `seq_lengths`: one sequence has exactly 65536 tokens; the live slots of all sequences together number at most half of the 4096 pages.
All inputs are finite; a program needn't handle non-finite values.
Results may differ from the reference program's by a relative error of at most 0.008.
Values may be sent and summed in bfloat16 or wider, within the bound.
A program may use at most 64 MiB of HBM per device.

```python
import math
import jax
import jax.numpy as jnp
from jax import lax

HQ = 64
KVH = 8
HD = 128
PAGE = 64
SEQS = 64
P_DEV = 128
POOL = 4096
MAXP = 1024
N_SEQ = 32


def page_layout(key):
    base = jax.random.fold_in(key, 7)
    keys_list = jax.random.split(base, 5)
    longest = jax.random.randint(keys_list[0], (), 0, SEQS)
    upper = max(1, POOL // (4 * (SEQS - 1)))
    seq_index = jnp.arange(SEQS, dtype=jnp.int32)
    page_count = jax.random.randint(keys_list[1], (SEQS,), 1, upper + 1)
    page_count = jnp.where(seq_index == longest, MAXP, page_count).astype(jnp.int32)
    last_fill = jax.random.randint(keys_list[2], (SEQS,), 1, PAGE + 1)
    last_fill = jnp.where(seq_index == longest, PAGE, last_fill).astype(jnp.int32)
    lengths = (page_count - 1) * PAGE + last_fill
    slot_ids = jnp.arange(MAXP, dtype=jnp.int32)
    used = (slot_ids[None, :] < page_count[:, None]).reshape(-1).astype(jnp.int32)
    ordinal = jnp.cumsum(used) - 1
    device_weight = jax.random.randint(keys_list[3], (N_SEQ,), 1, 17)
    raw_score = jax.random.randint(keys_list[4], (POOL,), 0, 65536)
    pool_ids = jnp.arange(POOL, dtype=jnp.int32)
    score = raw_score // device_weight[pool_ids // P_DEV] * POOL + pool_ids
    pool_order = jnp.argsort(score).astype(jnp.int32)
    target = pool_order[jnp.clip(ordinal, 0, POOL - 1)]
    target = jnp.where(used > 0, target, 0).reshape(SEQS, MAXP)
    return (lengths.astype(jnp.int32), (target // P_DEV).astype(jnp.int32), (target % P_DEV).astype(jnp.int32))


def draw_seq_lengths(key, part):
    return page_layout(key)[0]


def draw_page_owner(key, part):
    return page_layout(key)[1]


def draw_page_local(key, part):
    return page_layout(key)[2]


def draw_queries(key, part):
    values = jax.random.truncated_normal(key, -4.0, 4.0, (SEQS, HQ, HD), jnp.float32)
    row_scale = jnp.exp(jax.random.uniform(jax.random.fold_in(key, 3), (SEQS, 1, 1), jnp.float32, -0.7, 0.7))
    return (values * row_scale).astype(jnp.bfloat16)


def block_levels(key, dims, cuts, smallest, top_value):
    gain = 1.0
    for axis_at, parts in cuts:
        draws = jax.random.uniform(jax.random.fold_in(jax.random.fold_in(key, 6), axis_at), (parts,), jnp.float32, smallest / len(cuts), top_value / len(cuts))
        gain = gain * jnp.repeat(jnp.exp(draws), dims[axis_at] // parts).reshape((-1,) + (1,) * (len(dims) - 1 - axis_at))
    return gain


def bell_draw(rng, extent, scale, most, cuts=(), kind=jnp.bfloat16):
    loudness = block_levels(rng, extent, cuts, -0.22, 0.18) if cuts else 1.0
    values = jax.random.normal(rng, extent, jnp.float32) * scale * loudness
    return jnp.minimum(jnp.maximum(values, -most), most).astype(kind)


def setup_inputs(seed: int = 0, part: int = 0) -> dict:
    arg_keys = jax.random.split(jax.random.key(seed), 7)
    own_keys = jax.random.split(jax.random.fold_in(arg_keys[6], part), 7)
    queries = draw_queries(jax.random.fold_in(jax.random.fold_in(arg_keys[6], part), 71), part)
    key_pages = bell_draw(own_keys[1], (POOL, KVH, PAGE, HD), 1.0, 4.0, ((0, 32), (1, 8)))
    value_pages = bell_draw(own_keys[2], (POOL, KVH, PAGE, HD), 1.0, 6.0, ((0, 32), (1, 8)))
    page_owner = draw_page_owner(jax.random.fold_in(jax.random.fold_in(arg_keys[6], part), 71), part)
    page_local = draw_page_local(jax.random.fold_in(jax.random.fold_in(arg_keys[6], part), 71), part)
    seq_lengths = draw_seq_lengths(jax.random.fold_in(jax.random.fold_in(arg_keys[6], part), 71), part)
    return dict(queries=queries, key_pages=key_pages, value_pages=value_pages, page_owner=page_owner, page_local=page_local, seq_lengths=seq_lengths)


score_shift = 8.0

def reference(queries, key_pages, value_pages, page_owner, page_local, seq_lengths):
    group_size = HQ // KVH
    slot_ids = jnp.arange(MAXP, dtype=jnp.int32)
    slot_fill = jnp.clip(seq_lengths[:, None] - slot_ids[None, :] * PAGE, 0, PAGE).astype(jnp.int32)
    pool_index = (page_owner * P_DEV + page_local).astype(jnp.int32)
    target = jnp.where(slot_fill > 0, pool_index, POOL).astype(jnp.int32).reshape(-1)
    seq_ids = jnp.broadcast_to(jnp.arange(SEQS, dtype=jnp.int32)[:, None], (SEQS, MAXP)).reshape(-1)
    page_seq = jnp.zeros((POOL,), jnp.int32).at[target].set(seq_ids, mode='drop')
    page_fill = jnp.zeros((POOL,), jnp.int32).at[target].set(slot_fill.reshape(-1), mode='drop')
    block_pages = math.gcd(POOL, 64)
    block_count = POOL // block_pages
    key_blocks = key_pages.reshape(block_count, block_pages, KVH, PAGE, HD)
    value_blocks = value_pages.reshape(block_count, block_pages, KVH, PAGE, HD)
    seq_blocks = page_seq.reshape(block_count, block_pages)
    fill_blocks = page_fill.reshape(block_count, block_pages)
    score_scale = 1.0 / math.sqrt(HD)

    def visit(carry, block):
        numerator, denominator = carry
        key_block, value_block, seq_block, fill_block = block
        picked = queries[seq_block].astype(jnp.float32).reshape(block_pages, KVH, group_size, HD)
        scores = jnp.einsum('pkgd,pktd->pkgt', picked, key_block.astype(jnp.float32), precision=lax.Precision.HIGHEST) * score_scale
        live_mask = jnp.arange(PAGE, dtype=jnp.int32)[None, :] < fill_block[:, None]
        weight = jnp.where(live_mask[:, None, None, :], jnp.exp(scores - score_shift), 0.0)
        page_total = lax.optimization_barrier(jnp.sum(weight, axis=-1))
        rounded = lax.optimization_barrier(weight.astype(jnp.bfloat16)).astype(jnp.float32)
        page_sum = jnp.einsum('pkgt,pktd->pkgd', rounded, value_block.astype(jnp.float32), precision=lax.Precision.HIGHEST)
        numerator = numerator + jax.ops.segment_sum(page_sum, seq_block, num_segments=SEQS)
        denominator = denominator + jax.ops.segment_sum(page_total, seq_block, num_segments=SEQS)
        return ((numerator, denominator), None)
    start = (jnp.zeros((SEQS, KVH, group_size, HD), jnp.float32), jnp.zeros((SEQS, KVH, group_size), jnp.float32))
    (numerator, denominator), _ = lax.scan(visit, start, (key_blocks, value_blocks, seq_blocks, fill_blocks))
    result = numerator / denominator[..., None]
    return result.reshape(SEQS, HQ, HD).astype(jnp.bfloat16)
```

```python
import functools
import math

import jax
import jax.numpy as jnp
from jax import lax
from jax.experimental import pallas as pl
from jax.experimental.pallas import tpu as pltpu
from jax.sharding import PartitionSpec as P

SHIFT = 8.0
PHASE_ROWS = 128
LANES = 128
HI = 8
MESH = pl.DeviceIdType.MESH


def kernel(
    n,
    q_hbm,
    k_hbm,
    v_hbm,
    own_hbm,
    loc_hbm,
    len_ref,
    o_ref,
    q_buf,
    k_buf,
    v_buf,
    own_buf,
    loc_buf,
    q_all,
    tok_seq,
    num_out,
    tot_out,
    num_in,
    tot_in,
    load_sem,
    low_send,
    up_send,
    up2_send,
    q_recv,
    num_send,
    tot_send,
    num_recv,
    tot_recv,
    up_here,
    up2_here,
):
    z = lax.axis_index("seq")
    tp = lax.axis_index("tp")
    per, _, head_dim = q_buf.shape
    heads = q_all.shape[1] // per
    rows = per * heads
    seqs, slots = own_buf.shape
    tokens = k_buf.shape[0]
    chunk = tokens // HI
    page = k_buf.shape[0] // (HI * (LANES // HI))
    lows = LANES // HI
    devs = PHASE_ROWS // rows
    phases = n // devs

    loads = [
        pltpu.make_async_copy(src, dst, load_sem.at[i])
        for i, (src, dst) in enumerate(
            [(q_hbm, q_buf), (own_hbm, own_buf), (loc_hbm, loc_buf), (k_hbm, k_buf), (v_hbm, v_buf)]
        )
    ]
    for load in loads:
        load.start()

    barrier = pltpu.get_barrier_semaphore()

    def greet(d, carry):
        pl.semaphore_signal(barrier, inc=1, device_id={"seq": d}, device_id_type=MESH)
        return carry

    lax.fori_loop(z + 1, n, greet, 0)

    @pl.when(z >= 1)
    def _():
        pl.semaphore_wait(barrier, z)
        pl.semaphore_signal(up_here, inc=1, device_id={"seq": z - 1}, device_id_type=MESH)

    @pl.when(z >= 2)
    def _():
        pl.semaphore_signal(up2_here, inc=1, device_id={"seq": z - 2}, device_id_type=MESH)

    loads[0].wait()
    mine = jnp.zeros((per, heads, head_dim), jnp.float32)
    wide = q_buf[...].astype(jnp.float32)
    for t in range(q_buf.shape[1] // heads):
        mine = jnp.where(tp == t, wide[:, t * heads : (t + 1) * heads, :], mine)
    q_all[z] = mine.reshape(rows, head_dim).astype(jnp.bfloat16)

    def q_copy(j, d, sem):
        return pltpu.make_async_remote_copy(
            src_ref=q_all.at[j],
            dst_ref=q_all.at[j],
            send_sem=sem,
            recv_sem=q_recv.at[j],
            device_id={"seq": d},
            device_id_type=MESH,
        )

    def send_low(i, carry):
        d = z - 1 - i
        q_copy(z, d, low_send.at[d]).start()
        return carry

    lax.fori_loop(0, z, send_low, 0)

    loads[1].wait()
    loads[2].wait()
    slot = lax.broadcasted_iota(jnp.int32, (8, slots), 1)
    sub = lax.broadcasted_iota(jnp.int32, (8, slots), 0)

    def tally(g, table):
        own = own_buf[pl.ds(pl.multiple_of(g * 8, 8), 8), :]
        loc = loc_buf[pl.ds(pl.multiple_of(g * 8, 8), 8), :]
        length = jnp.zeros((8, slots), jnp.int32)
        for i in range(8):
            length = jnp.where(sub == i, len_ref[g * 8 + i], length)
        fill = jnp.clip(length - slot * page, 0, page)
        key = jnp.where((own == z) & (fill > 0), loc, -1)
        high = key >> (lows.bit_length() - 1)
        low = key & (lows - 1)
        fill_f = fill.astype(jnp.float32)
        seq_f = (g * 8 + sub).astype(jnp.float32)
        left = [jnp.where(high == h, v, 0.0) for v in (seq_f, fill_f) for h in range(HI)]
        right = [jnp.where(low == l, 1.0, 0.0) for l in range(lows)]
        left = jnp.concatenate(left, axis=0).astype(jnp.bfloat16)
        right = jnp.concatenate(right, axis=0).astype(jnp.bfloat16)
        return table + lax.dot_general(
            left, right, (((1,), (1,)), ((), ())), preferred_element_type=jnp.float32
        )

    table = lax.fori_loop(0, seqs // 8, tally, jnp.zeros((2 * HI * 8, lows * 8), jnp.float32))
    row_id = lax.broadcasted_iota(jnp.int32, table.shape, 0)
    col_id = lax.broadcasted_iota(jnp.int32, table.shape, 1)
    table = jnp.where((row_id & 7) == (col_id & 7), table, 0.0).astype(jnp.bfloat16)
    pick = (
        lax.broadcasted_iota(jnp.int32, (2 * HI, 2 * HI * 8), 1) >> 3
        == lax.broadcasted_iota(jnp.int32, (2 * HI, 2 * HI * 8), 0)
    )
    spread = (
        lax.broadcasted_iota(jnp.int32, (lows * 8, chunk), 0) >> 3
        == lax.broadcasted_iota(jnp.int32, (lows * 8, chunk), 1) // page
    )
    pick = jnp.where(pick, 1.0, 0.0).astype(jnp.bfloat16)
    spread = jnp.where(spread, 1.0, 0.0).astype(jnp.bfloat16)
    small = jnp.dot(pick, table, preferred_element_type=jnp.float32).astype(jnp.bfloat16)
    per_token = jnp.dot(small, spread, preferred_element_type=jnp.float32)
    place = (lax.broadcasted_iota(jnp.int32, (HI, chunk), 1) % page).astype(jnp.float32)
    tok_seq[...] = jnp.where(place < per_token[HI:], per_token[:HI], -1.0)

    @pl.when(z + 1 < n)
    def _():
        pl.semaphore_wait(up_here, 1)
        q_copy(z, z + 1, up_send).start()

    @pl.when(z + 2 < n)
    def _():
        pl.semaphore_wait(up2_here, 1)

        def pass_on(j, carry):
            q_copy(j, z, up_send).wait_recv()
            q_copy(j, z + 2, up2_send.at[j]).start()
            return carry

        lax.fori_loop(0, z, pass_on, 0)
        q_copy(z, z + 2, up2_send.at[z]).start()

    loads[3].wait()
    loads[4].wait()

    def num_copy(d, s):
        return pltpu.make_async_remote_copy(
            src_ref=num_out.at[d],
            dst_ref=num_in.at[s],
            send_sem=num_send.at[d],
            recv_sem=num_recv.at[s],
            device_id={"seq": d},
            device_id_type=MESH,
        )

    def tot_copy(d, s):
        return pltpu.make_async_remote_copy(
            src_ref=tot_out.at[d // devs],
            dst_ref=tot_in.at[s],
            send_sem=tot_send.at[d],
            recv_sem=tot_recv.at[s],
            device_id={"seq": d},
            device_id_type=MESH,
        )

    log2e = math.log2(math.e)
    gain, lift = log2e / math.sqrt(head_dim), SHIFT * log2e
    eye = lax.broadcasted_iota(jnp.int32, (PHASE_ROWS, LANES), 0) == lax.broadcasted_iota(
        jnp.int32, (PHASE_ROWS, LANES), 1
    )

    def phase(g, carry):
        def arrived(i, carry):
            j = g * devs + i

            @pl.when((j > z) | ((j < z) & (z + 2 >= n)))
            def _():
                q_copy(j, z, up_send).wait_recv()

            return carry

        lax.fori_loop(0, devs, arrived, 0)
        q = q_all[pl.ds(g * devs, devs)].reshape(PHASE_ROWS, head_dim)
        first = g * (devs * per)
        row_seq = (
            first + lax.broadcasted_iota(jnp.int32, (PHASE_ROWS, chunk), 0) // heads
        ).astype(jnp.float32)

        def tile(c, sums):
            num, tot = sums
            at = pl.ds(pl.multiple_of(c * chunk, chunk), chunk)
            s = lax.dot_general(
                q, k_buf[at, :], (((1,), (1,)), ((), ())), preferred_element_type=jnp.float32
            )
            w = jnp.exp2(s * gain - lift)
            w = jnp.where(tok_seq[pl.ds(c, 1), :] == row_seq, w, 0.0)
            for i in range(chunk // LANES):
                tot = tot + w[:, i * LANES : (i + 1) * LANES]
            num = num + jnp.dot(
                w.astype(jnp.bfloat16), v_buf[at, :], preferred_element_type=jnp.float32
            )
            return num, tot

        zero = jnp.zeros((PHASE_ROWS, LANES), jnp.float32)
        num, tot = lax.fori_loop(0, HI, tile, (zero, zero))
        num_out[pl.ds(g * devs, devs)] = num.astype(jnp.bfloat16).reshape(devs, rows, head_dim)
        tot = jnp.sum(tot, axis=1, keepdims=True)
        tot_out[g] = jnp.sum(jnp.where(eye, tot, 0.0), axis=0, keepdims=True)

        def give(i, carry):
            d = g * devs + i

            @pl.when(d != z)
            def _():
                num_copy(d, z).start()
                tot_copy(d, z).start()

            @pl.when(d == z)
            def _():
                num_in[z] = num_out[z]
                tot_in[z] = tot_out[g]

            return carry

        lax.fori_loop(0, devs, give, 0)
        return carry

    lax.fori_loop(0, phases, phase, 0)

    def collect(s, carry):
        @pl.when(s != z)
        def _():
            num_copy(z, s).wait_recv()
            tot_copy(z, s).wait_recv()

        return carry

    lax.fori_loop(0, n, collect, 0)
    num = jnp.sum(num_in[...].astype(jnp.float32), axis=0)
    tot = jnp.sum(tot_in[...], axis=0)
    at = lax.broadcasted_iota(jnp.int32, (rows, LANES), 0) + lax.rem(z, devs) * rows
    tot = jnp.where(lax.broadcasted_iota(jnp.int32, (rows, LANES), 1) == at, tot, 0.0)
    o_ref[...] = (num / jnp.sum(tot, axis=1, keepdims=True)).astype(jnp.bfloat16)

    def drain(d, carry):
        @pl.when(d < z)
        def _():
            q_copy(z, d, low_send.at[d]).wait_send()

        @pl.when((z + 2 < n) & (d <= z))
        def _():
            q_copy(d, z, up2_send.at[d]).wait_send()

        @pl.when(d != z)
        def _():
            num_copy(d, z).wait_send()
            tot_copy(d, z).wait_send()

        return carry

    lax.fori_loop(0, n, drain, 0)

    @pl.when(z + 1 < n)
    def _():
        q_copy(z, z, up_send).wait_send()


def body(queries, key_pages, value_pages, page_owner, page_local, seq_lengths):
    n = lax.axis_size("seq")
    per, all_heads, head_dim = queries.shape
    pool, kv, page, _ = key_pages.shape
    heads = all_heads // lax.axis_size("tp")
    rows = per * heads
    seqs, slots = page_owner.shape
    devs = PHASE_ROWS // rows
    assert kv == 1 and pool == LANES and head_dim == LANES and seqs == n * per
    tokens = pool * page
    dma = pltpu.SemaphoreType.DMA
    out = pl.pallas_call(
        functools.partial(kernel, n),
        out_shape=jax.ShapeDtypeStruct((rows, head_dim), jnp.bfloat16),
        in_specs=[pl.BlockSpec(memory_space=pl.ANY)] * 5
        + [pl.BlockSpec(memory_space=pltpu.SMEM)],
        out_specs=pl.BlockSpec(memory_space=pltpu.VMEM),
        scratch_shapes=[
            pltpu.VMEM(queries.shape, jnp.bfloat16),
            pltpu.VMEM((tokens, head_dim), jnp.bfloat16),
            pltpu.VMEM((tokens, head_dim), jnp.bfloat16),
            pltpu.VMEM((seqs, slots), jnp.int32),
            pltpu.VMEM((seqs, slots), jnp.int32),
            pltpu.VMEM((n, rows, head_dim), jnp.bfloat16),
            pltpu.VMEM((HI, tokens // HI), jnp.float32),
            pltpu.VMEM((n, rows, head_dim), jnp.bfloat16),
            pltpu.VMEM((n // devs, 1, LANES), jnp.float32),
            pltpu.VMEM((n, rows, head_dim), jnp.bfloat16),
            pltpu.VMEM((n, 1, LANES), jnp.float32),
            dma((5,)),
            dma((n,)),
            dma,
            dma((n,)),
            dma((n,)),
            dma((n,)),
            dma((n,)),
            dma((n,)),
            dma((n,)),
            pltpu.SemaphoreType.REGULAR,
            pltpu.SemaphoreType.REGULAR,
        ],
        compiler_params=pltpu.CompilerParams(collective_id=0, has_side_effects=True),
        name="paged_attention",
    )(
        queries,
        key_pages.reshape(tokens, head_dim),
        value_pages.reshape(tokens, head_dim),
        page_owner,
        page_local,
        seq_lengths,
    )
    return out.reshape(per, heads, head_dim)


def solution(mesh):
    placed = (
        P(("rep", "seq"), None, None),
        P(("rep", "seq"), "tp", None, None),
        P(("rep", "seq"), "tp", None, None),
        P("rep", None),
        P("rep", None),
        P("rep"),
    )
    return jax.shard_map(
        body, mesh=mesh, in_specs=placed, out_specs=P(("rep", "seq"), "tp", None), check_vma=False
    )
```

```python
import functools
import math

import jax
import jax.numpy as jnp
from jax import lax
from jax.experimental import pallas as pl
from jax.experimental.pallas import tpu as pltpu
from jax.sharding import PartitionSpec as P

SHIFT = 8.0
PHASE_ROWS = 128
LANES = 128
HI = 8
DOWN = 3
WRAP = 5
MESH = pl.DeviceIdType.MESH


def kernel(
    n,
    q_hbm,
    k_hbm,
    v_hbm,
    own_hbm,
    loc_hbm,
    len_ref,
    o_ref,
    q_buf,
    k_buf,
    v_buf,
    own_buf,
    loc_buf,
    q_all,
    tok_seq,
    num_out,
    tot_out,
    num_in,
    tot_in,
    load_sem,
    down_first,
    down_send,
    up_send,
    up2_send,
    wrap_send,
    wrap_recv,
    q_recv,
    num_send,
    tot_send,
    num_recv,
    tot_recv,
    up_here,
    up2_here,
    wrap_here,
):
    z = lax.axis_index("seq")
    tp = lax.axis_index("tp")
    shift = jnp.where(lax.axis_index("rep") + tp == 0, 1, 0)
    me = lax.rem(z + n - shift, n)

    def at_place(p):
        return {"seq": lax.rem(p + shift, n)}

    per, _, head_dim = q_buf.shape
    heads = q_all.shape[1] // per
    rows = per * heads
    seqs, slots = own_buf.shape
    tokens = k_buf.shape[0]
    chunk = tokens // HI
    page = k_buf.shape[0] // (HI * (LANES // HI))
    lows = LANES // HI
    devs = PHASE_ROWS // rows
    phases = n // devs

    loads = [
        pltpu.make_async_copy(src, dst, load_sem.at[i])
        for i, (src, dst) in enumerate(
            [(q_hbm, q_buf), (own_hbm, own_buf), (loc_hbm, loc_buf), (k_hbm, k_buf), (v_hbm, v_buf)]
        )
    ]
    for load in loads:
        load.start()

    barrier = pltpu.get_barrier_semaphore()

    def greet(d, carry):
        pl.semaphore_signal(barrier, inc=1, device_id=at_place(d), device_id_type=MESH)
        return carry

    lax.fori_loop(me + 1, n, greet, 0)

    @pl.when(me >= 1)
    def _():
        pl.semaphore_wait(barrier, me)
        pl.semaphore_signal(up_here, inc=1, device_id=at_place(me - 1), device_id_type=MESH)

    @pl.when(me >= 2)
    def _():
        pl.semaphore_signal(up2_here, inc=1, device_id=at_place(me - 2), device_id_type=MESH)

    @pl.when(me >= n - WRAP)
    def _():
        pl.semaphore_signal(
            wrap_here.at[me - (n - WRAP)], inc=1, device_id=at_place(0), device_id_type=MESH
        )

    loads[0].wait()
    mine = jnp.zeros((per, heads, head_dim), jnp.float32)
    wide = q_buf[...].astype(jnp.float32)
    for t in range(q_buf.shape[1] // heads):
        mine = jnp.where(tp == t, wide[:, t * heads : (t + 1) * heads, :], mine)
    q_all[me] = mine.reshape(rows, head_dim).astype(jnp.bfloat16)

    def q_copy(j, d, sem):
        return pltpu.make_async_remote_copy(
            src_ref=q_all.at[j],
            dst_ref=q_all.at[j],
            send_sem=sem,
            recv_sem=q_recv.at[j],
            device_id=at_place(d),
            device_id_type=MESH,
        )

    for i in range(DOWN):

        @pl.when(me > i)
        def _():
            q_copy(me, me - 1 - i, down_first.at[i]).start()

    loads[1].wait()
    loads[2].wait()
    slot = lax.broadcasted_iota(jnp.int32, (8, slots), 1)
    sub = lax.broadcasted_iota(jnp.int32, (8, slots), 0)

    def tally(g, table):
        own = own_buf[pl.ds(pl.multiple_of(g * 8, 8), 8), :]
        loc = loc_buf[pl.ds(pl.multiple_of(g * 8, 8), 8), :]
        length = jnp.zeros((8, slots), jnp.int32)
        for i in range(8):
            length = jnp.where(sub == i, len_ref[g * 8 + i], length)
        fill = jnp.clip(length - slot * page, 0, page)
        key = jnp.where((own == z) & (fill > 0), loc, -1)
        high = key >> (lows.bit_length() - 1)
        low = key & (lows - 1)
        fill_f = fill.astype(jnp.float32)
        seq_f = (g * 8 + sub).astype(jnp.float32)
        left = [jnp.where(high == h, v, 0.0) for v in (seq_f, fill_f) for h in range(HI)]
        right = [jnp.where(low == l, 1.0, 0.0) for l in range(lows)]
        left = jnp.concatenate(left, axis=0).astype(jnp.bfloat16)
        right = jnp.concatenate(right, axis=0).astype(jnp.bfloat16)
        return table + lax.dot_general(
            left, right, (((1,), (1,)), ((), ())), preferred_element_type=jnp.float32
        )

    table = lax.fori_loop(0, seqs // 8, tally, jnp.zeros((2 * HI * 8, lows * 8), jnp.float32))
    row_id = lax.broadcasted_iota(jnp.int32, table.shape, 0)
    col_id = lax.broadcasted_iota(jnp.int32, table.shape, 1)
    table = jnp.where((row_id & 7) == (col_id & 7), table, 0.0).astype(jnp.bfloat16)
    pick = (
        lax.broadcasted_iota(jnp.int32, (2 * HI, 2 * HI * 8), 1) >> 3
        == lax.broadcasted_iota(jnp.int32, (2 * HI, 2 * HI * 8), 0)
    )
    spread = (
        lax.broadcasted_iota(jnp.int32, (lows * 8, chunk), 0) >> 3
        == lax.broadcasted_iota(jnp.int32, (lows * 8, chunk), 1) // page
    )
    pick = jnp.where(pick, 1.0, 0.0).astype(jnp.bfloat16)
    spread = jnp.where(spread, 1.0, 0.0).astype(jnp.bfloat16)
    small = jnp.dot(pick, table, preferred_element_type=jnp.float32).astype(jnp.bfloat16)
    per_token = jnp.dot(small, spread, preferred_element_type=jnp.float32)
    place = (lax.broadcasted_iota(jnp.int32, (HI, chunk), 1) % page).astype(jnp.float32)
    tok_seq[...] = jnp.where(place < per_token[HI:], per_token[:HI], -1.0)

    @pl.when(me + 1 < n)
    def _():
        pl.semaphore_wait(up_here, 1)
        q_copy(me, me + 1, up_send).start()

    @pl.when(me + 2 < n)
    def _():
        pl.semaphore_wait(up2_here, 1)
        q_copy(me, me + 2, up2_send.at[me]).start()

    def wrap_copy(i, p):
        return pltpu.make_async_remote_copy(
            src_ref=q_all.at[pl.ds(0, devs)],
            dst_ref=q_all.at[pl.ds(0, devs)],
            send_sem=wrap_send.at[i],
            recv_sem=wrap_recv,
            device_id=at_place(p),
            device_id_type=MESH,
        )

    def goes_up(j):
        return (j < me) & (me + 2 < n) & ((j >= devs) | (me + 2 < n - WRAP))

    def goes_down(j):
        return (j > me) & (me >= DOWN)

    loads[3].wait()
    loads[4].wait()

    def num_copy(d, s):
        return pltpu.make_async_remote_copy(
            src_ref=num_out.at[d],
            dst_ref=num_in.at[s],
            send_sem=num_send.at[d],
            recv_sem=num_recv.at[s],
            device_id=at_place(d),
            device_id_type=MESH,
        )

    def tot_copy(d, s):
        return pltpu.make_async_remote_copy(
            src_ref=tot_out.at[d // devs],
            dst_ref=tot_in.at[s],
            send_sem=tot_send.at[d],
            recv_sem=tot_recv.at[s],
            device_id=at_place(d),
            device_id_type=MESH,
        )

    log2e = math.log2(math.e)
    gain, lift = log2e / math.sqrt(head_dim), SHIFT * log2e
    eye = lax.broadcasted_iota(jnp.int32, (PHASE_ROWS, LANES), 0) == lax.broadcasted_iota(
        jnp.int32, (PHASE_ROWS, LANES), 1
    )

    def phase(g, carry):
        @pl.when((g == 0) & (me >= n - WRAP))
        def _():
            wrap_copy(0, me).wait_recv()

        def arrived(i, carry):
            j = g * devs + i

            @pl.when((j != me) & ((g > 0) | (me < n - WRAP)))
            def _():
                q_copy(j, me, up_send).wait_recv()

            @pl.when(goes_up(j))
            def _():
                q_copy(j, me + 2, up2_send.at[j]).start()

            @pl.when(goes_down(j))
            def _():
                q_copy(j, me - DOWN, down_send.at[j]).start()

            return carry

        lax.fori_loop(0, devs, arrived, 0)
        q = q_all[pl.ds(g * devs, devs)].reshape(PHASE_ROWS, head_dim)
        row = lax.broadcasted_iota(jnp.int32, (PHASE_ROWS, 1), 0)
        source = g * devs + row // rows + shift
        source = jnp.where(source >= n, source - n, source)
        row_seq = (source * per + row % rows // heads).astype(jnp.float32)

        def tile(c, sums):
            num, tot = sums
            at = pl.ds(pl.multiple_of(c * chunk, chunk), chunk)
            s = lax.dot_general(
                q, k_buf[at, :], (((1,), (1,)), ((), ())), preferred_element_type=jnp.float32
            )
            w = jnp.exp2(s * gain - lift)
            w = jnp.where(tok_seq[pl.ds(c, 1), :] == row_seq, w, 0.0)
            for i in range(chunk // LANES):
                tot = tot + w[:, i * LANES : (i + 1) * LANES]
            num = num + jnp.dot(
                w.astype(jnp.bfloat16), v_buf[at, :], preferred_element_type=jnp.float32
            )
            return num, tot

        zero = jnp.zeros((PHASE_ROWS, LANES), jnp.float32)
        num, tot = lax.fori_loop(0, HI, tile, (zero, zero), unroll=2)
        num_out[pl.ds(g * devs, devs)] = num.astype(jnp.bfloat16).reshape(devs, rows, head_dim)
        tot = jnp.sum(tot, axis=1, keepdims=True)
        tot_out[g] = jnp.sum(jnp.where(eye, tot, 0.0), axis=0, keepdims=True)

        def give(i, carry):
            d = g * devs + i

            @pl.when(d != me)
            def _():
                num_copy(d, me).start()
                tot_copy(d, me).start()

            @pl.when(d == me)
            def _():
                num_in[me] = num_out[me]
                tot_in[me] = tot_out[g]

            return carry

        lax.fori_loop(0, devs, give, 0)

        @pl.when((g == 0) & (me == 0))
        def _():
            for i in range(WRAP):
                pl.semaphore_wait(wrap_here.at[i], 1)
                wrap_copy(i, n - WRAP + i).start()

        return carry

    lax.fori_loop(0, phases, phase, 0)

    def collect(s, carry):
        @pl.when(s != me)
        def _():
            num_copy(me, s).wait_recv()
            tot_copy(me, s).wait_recv()

        return carry

    lax.fori_loop(0, n, collect, 0)
    num = jnp.sum(num_in[...].astype(jnp.float32), axis=0)
    tot = jnp.sum(tot_in[...], axis=0)
    at = lax.broadcasted_iota(jnp.int32, (rows, LANES), 0) + lax.rem(me, devs) * rows
    tot = jnp.where(lax.broadcasted_iota(jnp.int32, (rows, LANES), 1) == at, tot, 0.0)
    o_ref[...] = (num / jnp.sum(tot, axis=1, keepdims=True)).astype(jnp.bfloat16)

    def drain(d, carry):
        @pl.when(goes_up(d) | ((d == me) & (me + 2 < n)))
        def _():
            q_copy(d, me, up2_send.at[d]).wait_send()

        @pl.when(goes_down(d))
        def _():
            q_copy(d, me, down_send.at[d]).wait_send()

        @pl.when(d != me)
        def _():
            num_copy(d, me).wait_send()
            tot_copy(d, me).wait_send()

        return carry

    lax.fori_loop(0, n, drain, 0)

    for i in range(DOWN):

        @pl.when(me > i)
        def _():
            q_copy(me, me, down_first.at[i]).wait_send()

    @pl.when(me + 1 < n)
    def _():
        q_copy(me, me, up_send).wait_send()

    @pl.when(me == 0)
    def _():
        for i in range(WRAP):
            wrap_copy(i, me).wait_send()


def body(queries, key_pages, value_pages, page_owner, page_local, seq_lengths):
    n = lax.axis_size("seq")
    per, all_heads, head_dim = queries.shape
    pool, kv, page, _ = key_pages.shape
    heads = all_heads // lax.axis_size("tp")
    rows = per * heads
    seqs, slots = page_owner.shape
    devs = PHASE_ROWS // rows
    assert kv == 1 and pool == LANES and head_dim == LANES and seqs == n * per
    tokens = pool * page
    dma = pltpu.SemaphoreType.DMA
    out = pl.pallas_call(
        functools.partial(kernel, n),
        out_shape=jax.ShapeDtypeStruct((rows, head_dim), jnp.bfloat16),
        in_specs=[pl.BlockSpec(memory_space=pl.ANY)] * 5
        + [pl.BlockSpec(memory_space=pltpu.SMEM)],
        out_specs=pl.BlockSpec(memory_space=pltpu.VMEM),
        scratch_shapes=[
            pltpu.VMEM(queries.shape, jnp.bfloat16),
            pltpu.VMEM((tokens, head_dim), jnp.bfloat16),
            pltpu.VMEM((tokens, head_dim), jnp.bfloat16),
            pltpu.VMEM((seqs, slots), jnp.int32),
            pltpu.VMEM((seqs, slots), jnp.int32),
            pltpu.VMEM((n, rows, head_dim), jnp.bfloat16),
            pltpu.VMEM((HI, tokens // HI), jnp.float32),
            pltpu.VMEM((n, rows, head_dim), jnp.bfloat16),
            pltpu.VMEM((n // devs, 1, LANES), jnp.float32),
            pltpu.VMEM((n, rows, head_dim), jnp.bfloat16),
            pltpu.VMEM((n, 1, LANES), jnp.float32),
            dma((5,)),
            dma((DOWN,)),
            dma((n,)),
            dma,
            dma((n,)),
            dma((WRAP,)),
            dma,
            dma((n,)),
            dma((n,)),
            dma((n,)),
            dma((n,)),
            dma((n,)),
            pltpu.SemaphoreType.REGULAR,
            pltpu.SemaphoreType.REGULAR,
            pltpu.SemaphoreType.REGULAR((WRAP,)),
        ],
        compiler_params=pltpu.CompilerParams(collective_id=0, has_side_effects=True),
        name="paged_attention",
    )(
        queries,
        key_pages.reshape(tokens, head_dim),
        value_pages.reshape(tokens, head_dim),
        page_owner,
        page_local,
        seq_lengths,
    )
    return out.reshape(per, heads, head_dim)


def solution(mesh):
    placed = (
        P(("rep", "seq"), None, None),
        P(("rep", "seq"), "tp", None, None),
        P(("rep", "seq"), "tp", None, None),
        P("rep", None),
        P("rep", None),
        P("rep"),
    )
    return jax.shard_map(
        body, mesh=mesh, in_specs=placed, out_specs=P(("rep", "seq"), "tp", None), check_vma=False
    )
```

```python
import functools
import math

import jax
import jax.numpy as jnp
from jax import lax
from jax.experimental import pallas as pl
from jax.experimental.pallas import tpu as pltpu
from jax.sharding import PartitionSpec as P

SHIFT = 8.0
PHASE_ROWS = 128
LANES = 128
HI = 8
WRAP = 5
WRAP_PHASES = 2
MESH = pl.DeviceIdType.MESH


def kernel(
    n,
    q_hbm,
    k_hbm,
    v_hbm,
    own_hbm,
    loc_hbm,
    len_ref,
    o_ref,
    q_buf,
    k_buf,
    v_buf,
    own_buf,
    loc_buf,
    q_all,
    tok_seq,
    num_out,
    tot_out,
    num_in,
    tot_in,
    load_sem,
    low_send,
    over_send,
    up_send,
    up2_send,
    wrap_send,
    wrap_recv,
    q_recv,
    num_send,
    tot_send,
    num_recv,
    tot_recv,
    up_here,
    up2_here,
    wrap_here,
):
    z = lax.axis_index("seq")
    tp = lax.axis_index("tp")
    shift = jnp.where(lax.axis_index("rep") + tp == 0, 1, 0)
    me = lax.rem(z + n - shift, n)

    def at_place(p):
        return {"seq": lax.rem(p + shift, n)}

    per, _, head_dim = q_buf.shape
    heads = q_all.shape[1] // per
    rows = per * heads
    seqs, slots = own_buf.shape
    tokens = k_buf.shape[0]
    chunk = tokens // HI
    page = k_buf.shape[0] // (HI * (LANES // HI))
    lows = LANES // HI
    devs = PHASE_ROWS // rows
    phases = n // devs

    loads = [
        pltpu.make_async_copy(src, dst, load_sem.at[i])
        for i, (src, dst) in enumerate(
            [(q_hbm, q_buf), (own_hbm, own_buf), (loc_hbm, loc_buf), (k_hbm, k_buf), (v_hbm, v_buf)]
        )
    ]
    for load in loads:
        load.start()

    barrier = pltpu.get_barrier_semaphore()

    def greet(d, carry):
        pl.semaphore_signal(barrier, inc=1, device_id=at_place(d), device_id_type=MESH)
        return carry

    lax.fori_loop(me + 1, n, greet, 0)

    @pl.when(me >= 1)
    def _():
        pl.semaphore_wait(barrier, me)
        pl.semaphore_signal(up_here, inc=1, device_id=at_place(me - 1), device_id_type=MESH)

    @pl.when(me >= 2)
    def _():
        pl.semaphore_signal(up2_here, inc=1, device_id=at_place(me - 2), device_id_type=MESH)

    @pl.when(me >= n - WRAP)
    def _():
        pl.semaphore_signal(
            wrap_here.at[me - (n - WRAP)], inc=1, device_id=at_place(0), device_id_type=MESH
        )

    loads[0].wait()
    mine = jnp.zeros((per, heads, head_dim), jnp.float32)
    wide = q_buf[...].astype(jnp.float32)
    for t in range(q_buf.shape[1] // heads):
        mine = jnp.where(tp == t, wide[:, t * heads : (t + 1) * heads, :], mine)
    q_all[me] = mine.reshape(rows, head_dim).astype(jnp.bfloat16)

    def q_copy(j, d, sem):
        return pltpu.make_async_remote_copy(
            src_ref=q_all.at[j],
            dst_ref=q_all.at[j],
            send_sem=sem,
            recv_sem=q_recv.at[j],
            device_id=at_place(d),
            device_id_type=MESH,
        )

    half = n // 2

    def far(j, p):
        return j - p > half

    @pl.when(far(me, 0))
    def _():
        q_copy(me, 0, over_send.at[0]).start()

    def send_low(d, carry):
        q_copy(me, d, low_send.at[d]).start()
        return carry

    lax.fori_loop(jnp.maximum(me - half, 0), me, send_low, 0)

    loads[1].wait()
    loads[2].wait()
    slot = lax.broadcasted_iota(jnp.int32, (8, slots), 1)
    sub = lax.broadcasted_iota(jnp.int32, (8, slots), 0)

    def tally(g, table):
        own = own_buf[pl.ds(pl.multiple_of(g * 8, 8), 8), :]
        loc = loc_buf[pl.ds(pl.multiple_of(g * 8, 8), 8), :]
        length = jnp.zeros((8, slots), jnp.int32)
        for i in range(8):
            length = jnp.where(sub == i, len_ref[g * 8 + i], length)
        fill = jnp.clip(length - slot * page, 0, page)
        key = jnp.where((own == z) & (fill > 0), loc, -1)
        high = key >> (lows.bit_length() - 1)
        low = key & (lows - 1)
        fill_f = fill.astype(jnp.float32)
        seq_f = (g * 8 + sub).astype(jnp.float32)
        left = [jnp.where(high == h, v, 0.0) for v in (seq_f, fill_f) for h in range(HI)]
        right = [jnp.where(low == l, 1.0, 0.0) for l in range(lows)]
        left = jnp.concatenate(left, axis=0).astype(jnp.bfloat16)
        right = jnp.concatenate(right, axis=0).astype(jnp.bfloat16)
        return table + lax.dot_general(
            left, right, (((1,), (1,)), ((), ())), preferred_element_type=jnp.float32
        )

    table = lax.fori_loop(0, seqs // 8, tally, jnp.zeros((2 * HI * 8, lows * 8), jnp.float32))
    row_id = lax.broadcasted_iota(jnp.int32, table.shape, 0)
    col_id = lax.broadcasted_iota(jnp.int32, table.shape, 1)
    table = jnp.where((row_id & 7) == (col_id & 7), table, 0.0).astype(jnp.bfloat16)
    pick = (
        lax.broadcasted_iota(jnp.int32, (2 * HI, 2 * HI * 8), 1) >> 3
        == lax.broadcasted_iota(jnp.int32, (2 * HI, 2 * HI * 8), 0)
    )
    spread = (
        lax.broadcasted_iota(jnp.int32, (lows * 8, chunk), 0) >> 3
        == lax.broadcasted_iota(jnp.int32, (lows * 8, chunk), 1) // page
    )
    pick = jnp.where(pick, 1.0, 0.0).astype(jnp.bfloat16)
    spread = jnp.where(spread, 1.0, 0.0).astype(jnp.bfloat16)
    small = jnp.dot(pick, table, preferred_element_type=jnp.float32).astype(jnp.bfloat16)
    per_token = jnp.dot(small, spread, preferred_element_type=jnp.float32)
    place = (lax.broadcasted_iota(jnp.int32, (HI, chunk), 1) % page).astype(jnp.float32)
    tok_seq[...] = jnp.where(place < per_token[HI:], per_token[:HI], -1.0)

    @pl.when(me + 1 < n)
    def _():
        pl.semaphore_wait(up_here, 1)
        q_copy(me, me + 1, up_send).start()

    @pl.when(me + 2 < n)
    def _():
        pl.semaphore_wait(up2_here, 1)
        q_copy(me, me + 2, up2_send.at[me]).start()

    def wrap_copy(g, i, p):
        return pltpu.make_async_remote_copy(
            src_ref=q_all.at[pl.ds(g * devs, devs)],
            dst_ref=q_all.at[pl.ds(g * devs, devs)],
            send_sem=wrap_send.at[g, i],
            recv_sem=wrap_recv.at[g],
            device_id=at_place(p),
            device_id_type=MESH,
        )

    def goes_up(j):
        return ((j < me) & (me + 2 < n) & ((j >= WRAP_PHASES * devs) | (me + 2 < n - WRAP))) | far(
            j, me + 2
        )

    loads[3].wait()
    loads[4].wait()

    def num_copy(d, s):
        return pltpu.make_async_remote_copy(
            src_ref=num_out.at[d],
            dst_ref=num_in.at[s],
            send_sem=num_send.at[d],
            recv_sem=num_recv.at[s],
            device_id=at_place(d),
            device_id_type=MESH,
        )

    def tot_copy(d, s):
        return pltpu.make_async_remote_copy(
            src_ref=tot_out.at[d // devs],
            dst_ref=tot_in.at[s],
            send_sem=tot_send.at[d],
            recv_sem=tot_recv.at[s],
            device_id=at_place(d),
            device_id_type=MESH,
        )

    log2e = math.log2(math.e)
    gain, lift = log2e / math.sqrt(head_dim), SHIFT * log2e
    eye = lax.broadcasted_iota(jnp.int32, (PHASE_ROWS, LANES), 0) == lax.broadcasted_iota(
        jnp.int32, (PHASE_ROWS, LANES), 1
    )

    def phase(g, carry):
        fed = (g < WRAP_PHASES) & (me >= n - WRAP)

        @pl.when(fed)
        def _():
            wrap_copy(g, 0, me).wait_recv()

        def arrived(j, carry):
            @pl.when((j != me) & jnp.logical_not(fed))
            def _():
                q_copy(j, me, up_send).wait_recv()

            @pl.when((me == 0) & far(j, 1))
            def _():
                q_copy(j, 1, over_send.at[j]).start()

            @pl.when(goes_up(j))
            def _():
                q_copy(j, me + 2, up2_send.at[j]).start()

            return carry

        start = g * devs
        stop = jnp.where(g < phases // 2, start + devs, jnp.where(g == phases // 2, n, start))
        lax.fori_loop(start, stop, arrived, 0)
        q = q_all[pl.ds(g * devs, devs)].reshape(PHASE_ROWS, head_dim)
        row = lax.broadcasted_iota(jnp.int32, (PHASE_ROWS, 1), 0)
        source = g * devs + row // rows + shift
        source = jnp.where(source >= n, source - n, source)
        row_seq = (source * per + row % rows // heads).astype(jnp.float32)

        def tile(c, sums):
            num, tot = sums
            at = pl.ds(pl.multiple_of(c * chunk, chunk), chunk)
            s = lax.dot_general(
                q, k_buf[at, :], (((1,), (1,)), ((), ())), preferred_element_type=jnp.float32
            )
            w = jnp.exp2(s * gain - lift)
            w = jnp.where(tok_seq[pl.ds(c, 1), :] == row_seq, w, 0.0)
            for i in range(chunk // LANES):
                tot = tot + w[:, i * LANES : (i + 1) * LANES]
            num = num + jnp.dot(
                w.astype(jnp.bfloat16), v_buf[at, :], preferred_element_type=jnp.float32
            )
            return num, tot

        zero = jnp.zeros((PHASE_ROWS, LANES), jnp.float32)
        num, tot = lax.fori_loop(0, HI, tile, (zero, zero), unroll=2)
        num_out[pl.ds(g * devs, devs)] = num.astype(jnp.bfloat16).reshape(devs, rows, head_dim)
        tot = jnp.sum(tot, axis=1, keepdims=True)
        tot_out[g] = jnp.sum(jnp.where(eye, tot, 0.0), axis=0, keepdims=True)

        def give(i, carry):
            d = g * devs + i

            @pl.when(d != me)
            def _():
                num_copy(d, me).start()
                tot_copy(d, me).start()

            @pl.when(d == me)
            def _():
                num_in[me] = num_out[me]
                tot_in[me] = tot_out[g]

            return carry

        lax.fori_loop(0, devs, give, 0)

        @pl.when((g == WRAP_PHASES - 1) & (me == 0))
        def _():
            for i in range(WRAP):
                pl.semaphore_wait(wrap_here.at[i], 1)
                wrap_copy(0, i, n - WRAP + i).start()
            for w in range(1, WRAP_PHASES):
                for i in range(WRAP):
                    wrap_copy(w, i, n - WRAP + i).start()

        return carry

    lax.fori_loop(0, phases, phase, 0)

    def collect(s, carry):
        @pl.when(s != me)
        def _():
            num_copy(me, s).wait_recv()
            tot_copy(me, s).wait_recv()

        return carry

    lax.fori_loop(0, n, collect, 0)
    num = jnp.sum(num_in[...].astype(jnp.float32), axis=0)
    tot = jnp.sum(tot_in[...], axis=0)
    at = lax.broadcasted_iota(jnp.int32, (rows, LANES), 0) + lax.rem(me, devs) * rows
    tot = jnp.where(lax.broadcasted_iota(jnp.int32, (rows, LANES), 1) == at, tot, 0.0)
    o_ref[...] = (num / jnp.sum(tot, axis=1, keepdims=True)).astype(jnp.bfloat16)

    def drain(d, carry):
        @pl.when(goes_up(d) | ((d == me) & (me + 2 < n)))
        def _():
            q_copy(d, me, up2_send.at[d]).wait_send()

        @pl.when((me == 0) & far(d, 1))
        def _():
            q_copy(d, me, over_send.at[d]).wait_send()

        @pl.when((d < me) & (d >= me - half))
        def _():
            q_copy(me, me, low_send.at[d]).wait_send()

        @pl.when(d != me)
        def _():
            num_copy(d, me).wait_send()
            tot_copy(d, me).wait_send()

        return carry

    lax.fori_loop(0, n, drain, 0)

    @pl.when(far(me, 0))
    def _():
        q_copy(me, me, over_send.at[0]).wait_send()

    @pl.when(me + 1 < n)
    def _():
        q_copy(me, me, up_send).wait_send()

    @pl.when(me == 0)
    def _():
        for w in range(WRAP_PHASES):
            for i in range(WRAP):
                wrap_copy(w, i, me).wait_send()


def body(queries, key_pages, value_pages, page_owner, page_local, seq_lengths):
    n = lax.axis_size("seq")
    per, all_heads, head_dim = queries.shape
    pool, kv, page, _ = key_pages.shape
    heads = all_heads // lax.axis_size("tp")
    rows = per * heads
    seqs, slots = page_owner.shape
    devs = PHASE_ROWS // rows
    assert kv == 1 and pool == LANES and head_dim == LANES and seqs == n * per
    tokens = pool * page
    dma = pltpu.SemaphoreType.DMA
    out = pl.pallas_call(
        functools.partial(kernel, n),
        out_shape=jax.ShapeDtypeStruct((rows, head_dim), jnp.bfloat16),
        in_specs=[pl.BlockSpec(memory_space=pl.ANY)] * 5
        + [pl.BlockSpec(memory_space=pltpu.SMEM)],
        out_specs=pl.BlockSpec(memory_space=pltpu.VMEM),
        scratch_shapes=[
            pltpu.VMEM(queries.shape, jnp.bfloat16),
            pltpu.VMEM((tokens, head_dim), jnp.bfloat16),
            pltpu.VMEM((tokens, head_dim), jnp.bfloat16),
            pltpu.VMEM((seqs, slots), jnp.int32),
            pltpu.VMEM((seqs, slots), jnp.int32),
            pltpu.VMEM((n, rows, head_dim), jnp.bfloat16),
            pltpu.VMEM((HI, tokens // HI), jnp.float32),
            pltpu.VMEM((n, rows, head_dim), jnp.bfloat16),
            pltpu.VMEM((n // devs, 1, LANES), jnp.float32),
            pltpu.VMEM((n, rows, head_dim), jnp.bfloat16),
            pltpu.VMEM((n, 1, LANES), jnp.float32),
            dma((5,)),
            dma((n,)),
            dma((n,)),
            dma,
            dma((n,)),
            dma((WRAP_PHASES, WRAP)),
            dma((WRAP_PHASES,)),
            dma((n,)),
            dma((n,)),
            dma((n,)),
            dma((n,)),
            dma((n,)),
            pltpu.SemaphoreType.REGULAR,
            pltpu.SemaphoreType.REGULAR,
            pltpu.SemaphoreType.REGULAR((WRAP,)),
        ],
        compiler_params=pltpu.CompilerParams(collective_id=0, has_side_effects=True),
        name="paged_attention",
    )(
        queries,
        key_pages.reshape(tokens, head_dim),
        value_pages.reshape(tokens, head_dim),
        page_owner,
        page_local,
        seq_lengths,
    )
    return out.reshape(per, heads, head_dim)


def solution(mesh):
    placed = (
        P(("rep", "seq"), None, None),
        P(("rep", "seq"), "tp", None, None),
        P(("rep", "seq"), "tp", None, None),
        P("rep", None),
        P("rep", None),
        P("rep"),
    )
    return jax.shard_map(
        body, mesh=mesh, in_specs=placed, out_specs=P(("rep", "seq"), "tp", None), check_vma=False
    )
```

```python
import functools
import math

import jax
import jax.numpy as jnp
from jax import lax
from jax.experimental import pallas as pl
from jax.experimental.pallas import tpu as pltpu
from jax.sharding import PartitionSpec as P

SHIFT = 8.0
PHASE_ROWS = 128
LANES = 128
HI = 8
WRAP = 8
WRAP_PHASES = 2
MESH = pl.DeviceIdType.MESH


def kernel(
    n,
    q_hbm,
    k_hbm,
    v_hbm,
    own_hbm,
    loc_hbm,
    len_hbm,
    o_ref,
    q_buf,
    k_buf,
    v_buf,
    own_buf,
    loc_buf,
    len_ref,
    q_all,
    tok_seq,
    num_out,
    tot_out,
    num_in,
    tot_in,
    load_sem,
    low_send,
    up_send,
    up2_send,
    wrap_send,
    wrap_recv,
    q_recv,
    num_send,
    tot_send,
    num_recv,
    tot_recv,
    up_here,
    up2_here,
    wrap_here,
):
    z = lax.axis_index("seq")
    tp = lax.axis_index("tp")
    shift = jnp.where(lax.axis_index("rep") + tp == 0, 1, 0)
    me = lax.rem(z + n - shift, n)

    def at_place(p):
        return {"seq": lax.rem(p + shift, n)}

    per, _, head_dim = q_buf.shape
    heads = q_all.shape[1] // per
    rows = per * heads
    seqs, slots = own_buf.shape
    tokens = k_buf.shape[0]
    chunk = tokens // HI
    page = k_buf.shape[0] // (HI * (LANES // HI))
    lows = LANES // HI
    devs = PHASE_ROWS // rows
    phases = n // devs

    loads = [
        pltpu.make_async_copy(src, dst, load_sem.at[i])
        for i, (src, dst) in enumerate(
            [
                (q_hbm, q_buf),
                (own_hbm, own_buf),
                (loc_hbm, loc_buf),
                (k_hbm, k_buf),
                (v_hbm, v_buf),
                (len_hbm, len_ref),
            ]
        )
    ]
    for load in loads:
        load.start()

    barrier = pltpu.get_barrier_semaphore()

    def greet(d, carry):
        pl.semaphore_signal(barrier, inc=1, device_id=at_place(d), device_id_type=MESH)
        return carry

    lax.fori_loop(me + 1, n, greet, 0)

    @pl.when(me >= 1)
    def _():
        pl.semaphore_wait(barrier, me)
        pl.semaphore_signal(up_here, inc=1, device_id=at_place(me - 1), device_id_type=MESH)

    @pl.when(me >= 2)
    def _():
        pl.semaphore_signal(up2_here, inc=1, device_id=at_place(me - 2), device_id_type=MESH)

    @pl.when(me >= n - WRAP)
    def _():
        pl.semaphore_signal(
            wrap_here.at[me - (n - WRAP)], inc=1, device_id=at_place(0), device_id_type=MESH
        )

    loads[0].wait()
    mine = jnp.zeros((per, heads, head_dim), jnp.float32)
    wide = q_buf[...].astype(jnp.float32)
    for t in range(q_buf.shape[1] // heads):
        mine = jnp.where(tp == t, wide[:, t * heads : (t + 1) * heads, :], mine)
    q_all[me] = mine.reshape(rows, head_dim).astype(jnp.bfloat16)

    def q_copy(j, d, sem):
        return pltpu.make_async_remote_copy(
            src_ref=q_all.at[j],
            dst_ref=q_all.at[j],
            send_sem=sem,
            recv_sem=q_recv.at[j],
            device_id=at_place(d),
            device_id_type=MESH,
        )

    half = n // 2

    def far(j, p):
        return j - p > half

    @pl.when(far(me, 0))
    def _():
        q_copy(me, 0, low_send.at[0]).start()

    def send_low(d, carry):
        q_copy(me, d, low_send.at[d]).start()
        return carry

    lax.fori_loop(jnp.maximum(me - half, 0), me, send_low, 0)

    loads[1].wait()
    loads[2].wait()
    loads[5].wait()
    slot = lax.broadcasted_iota(jnp.int32, (8, slots), 1)
    sub = lax.broadcasted_iota(jnp.int32, (8, slots), 0)

    def tally(g, table):
        own = own_buf[pl.ds(pl.multiple_of(g * 8, 8), 8), :]
        loc = loc_buf[pl.ds(pl.multiple_of(g * 8, 8), 8), :]
        length = jnp.zeros((8, slots), jnp.int32)
        for i in range(8):
            length = jnp.where(sub == i, len_ref[g * 8 + i], length)
        fill = jnp.clip(length - slot * page, 0, page)
        key = jnp.where((own == z) & (fill > 0), loc, -1)
        high = key >> (lows.bit_length() - 1)
        low = key & (lows - 1)
        fill_f = fill.astype(jnp.float32)
        seq_f = (g * 8 + sub).astype(jnp.float32)
        left = [jnp.where(high == h, v, 0.0) for v in (seq_f, fill_f) for h in range(HI)]
        right = [jnp.where(low == l, 1.0, 0.0) for l in range(lows)]
        left = jnp.concatenate(left, axis=0).astype(jnp.bfloat16)
        right = jnp.concatenate(right, axis=0).astype(jnp.bfloat16)
        return table + lax.dot_general(
            left, right, (((1,), (1,)), ((), ())), preferred_element_type=jnp.float32
        )

    table = lax.fori_loop(0, seqs // 8, tally, jnp.zeros((2 * HI * 8, lows * 8), jnp.float32))
    row_id = lax.broadcasted_iota(jnp.int32, table.shape, 0)
    col_id = lax.broadcasted_iota(jnp.int32, table.shape, 1)
    table = jnp.where((row_id & 7) == (col_id & 7), table, 0.0).astype(jnp.bfloat16)
    pick = (
        lax.broadcasted_iota(jnp.int32, (2 * HI, 2 * HI * 8), 1) >> 3
        == lax.broadcasted_iota(jnp.int32, (2 * HI, 2 * HI * 8), 0)
    )
    spread = (
        lax.broadcasted_iota(jnp.int32, (lows * 8, chunk), 0) >> 3
        == lax.broadcasted_iota(jnp.int32, (lows * 8, chunk), 1) // page
    )
    pick = jnp.where(pick, 1.0, 0.0).astype(jnp.bfloat16)
    spread = jnp.where(spread, 1.0, 0.0).astype(jnp.bfloat16)
    small = jnp.dot(pick, table, preferred_element_type=jnp.float32).astype(jnp.bfloat16)
    per_token = jnp.dot(small, spread, preferred_element_type=jnp.float32)
    place = (lax.broadcasted_iota(jnp.int32, (HI, chunk), 1) % page).astype(jnp.float32)
    tok_seq[...] = jnp.where(place < per_token[HI:], per_token[:HI], -1.0)

    @pl.when(me + 1 < n)
    def _():
        pl.semaphore_wait(up_here, 1)
        q_copy(me, me + 1, up_send).start()

    @pl.when(me + 2 < n)
    def _():
        pl.semaphore_wait(up2_here, 1)
        q_copy(me, me + 2, up2_send.at[me]).start()

    def wrap_copy(g, i, p):
        return pltpu.make_async_remote_copy(
            src_ref=q_all.at[pl.ds(g * devs, devs)],
            dst_ref=q_all.at[pl.ds(g * devs, devs)],
            send_sem=wrap_send.at[g, i],
            recv_sem=wrap_recv.at[g],
            device_id=at_place(p),
            device_id_type=MESH,
        )

    def goes_up(j):
        return ((j < me) & (me + 2 < n) & ((j >= WRAP_PHASES * devs) | (me + 2 < n - WRAP))) | far(
            j, me + 2
        )

    loads[3].wait()
    loads[4].wait()

    def num_copy(d, s):
        return pltpu.make_async_remote_copy(
            src_ref=num_out.at[d],
            dst_ref=num_in.at[s],
            send_sem=num_send,
            recv_sem=num_recv,
            device_id=at_place(d),
            device_id_type=MESH,
        )

    def tot_copy(d, s):
        return pltpu.make_async_remote_copy(
            src_ref=tot_out.at[d // devs],
            dst_ref=tot_in.at[s],
            send_sem=tot_send,
            recv_sem=tot_recv,
            device_id=at_place(d),
            device_id_type=MESH,
        )

    def all_copies(src, dst, send, recv):
        return pltpu.make_async_remote_copy(
            src_ref=src.at[pl.ds(0, n - 1)],
            dst_ref=dst.at[pl.ds(0, n - 1)],
            send_sem=send,
            recv_sem=recv,
            device_id=at_place(me),
            device_id_type=MESH,
        )

    all_num = all_copies(num_in, num_in, num_send, num_recv)
    all_tot = all_copies(tot_in, tot_in, tot_send, tot_recv)

    log2e = math.log2(math.e)
    gain, lift = log2e / math.sqrt(head_dim), SHIFT * log2e
    eye = lax.broadcasted_iota(jnp.int32, (PHASE_ROWS, LANES), 0) == lax.broadcasted_iota(
        jnp.int32, (PHASE_ROWS, LANES), 1
    )

    def phase(g, carry):
        fed = (g < WRAP_PHASES) & (me >= n - WRAP)

        @pl.when(fed)
        def _():
            wrap_copy(g, 0, me).wait_recv()

        def arrived(j, carry):
            @pl.when((j != me) & jnp.logical_not(fed))
            def _():
                q_copy(j, me, up_send).wait_recv()

            @pl.when((me == 0) & far(j, 1))
            def _():
                q_copy(j, 1, low_send.at[j]).start()

            @pl.when(goes_up(j))
            def _():
                q_copy(j, me + 2, up2_send.at[j]).start()

            return carry

        start = g * devs
        stop = jnp.where(g < phases // 2, start + devs, jnp.where(g == phases // 2, n, start))
        lax.fori_loop(start, stop, arrived, 0)
        @pl.when((g == WRAP_PHASES - 1) & (me == 0))
        def _():
            for i in range(WRAP):
                pl.semaphore_wait(wrap_here.at[i], 1)
                wrap_copy(0, i, n - WRAP + i).start()
            for w in range(1, WRAP_PHASES):
                for i in range(WRAP):
                    wrap_copy(w, i, n - WRAP + i).start()

        q = q_all[pl.ds(g * devs, devs)].reshape(PHASE_ROWS, head_dim)
        row = lax.broadcasted_iota(jnp.int32, (PHASE_ROWS, 1), 0)
        source = g * devs + row // rows + shift
        source = jnp.where(source >= n, source - n, source)
        row_seq = (source * per + row % rows // heads).astype(jnp.float32)

        def tile(c, sums):
            num, tot = sums
            at = pl.ds(pl.multiple_of(c * chunk, chunk), chunk)
            s = lax.dot_general(
                q, k_buf[at, :], (((1,), (1,)), ((), ())), preferred_element_type=jnp.float32
            )
            w = jnp.exp2(s * gain - lift)
            w = jnp.where(tok_seq[pl.ds(c, 1), :] == row_seq, w, 0.0)
            for i in range(chunk // LANES):
                tot = tot + w[:, i * LANES : (i + 1) * LANES]
            num = num + jnp.dot(
                w.astype(jnp.bfloat16), v_buf[at, :], preferred_element_type=jnp.float32
            )
            return num, tot

        zero = jnp.zeros((PHASE_ROWS, LANES), jnp.float32)
        num, tot = lax.fori_loop(0, HI, tile, (zero, zero), unroll=2)
        num_out[pl.ds(g * devs, devs)] = num.astype(jnp.bfloat16).reshape(devs, rows, head_dim)
        tot = jnp.sum(tot, axis=1, keepdims=True)
        tot_out[g] = jnp.sum(jnp.where(eye, tot, 0.0), axis=0, keepdims=True)

        def give(i, carry):
            d = g * devs + i

            @pl.when(d != me)
            def _():
                num_copy(d, me).start()
                tot_copy(d, me).start()

            @pl.when(d == me)
            def _():
                num_in[me] = num_out[me]
                tot_in[me] = tot_out[g]

            return carry

        lax.fori_loop(0, devs, give, 0)

        return carry

    lax.fori_loop(0, phases, phase, 0)

    all_num.wait_recv()
    all_tot.wait_recv()
    num = jnp.sum(num_in[...].astype(jnp.float32), axis=0)
    tot = jnp.sum(tot_in[...], axis=0)
    at = lax.broadcasted_iota(jnp.int32, (rows, LANES), 0) + lax.rem(me, devs) * rows
    tot = jnp.where(lax.broadcasted_iota(jnp.int32, (rows, LANES), 1) == at, tot, 0.0)
    o_ref[...] = (num / jnp.sum(tot, axis=1, keepdims=True)).astype(jnp.bfloat16)

    def drain(d, carry):
        @pl.when(goes_up(d) | ((d == me) & (me + 2 < n)))
        def _():
            q_copy(d, me, up2_send.at[d]).wait_send()

        @pl.when((me == 0) & far(d, 1))
        def _():
            q_copy(d, me, low_send.at[d]).wait_send()

        @pl.when((d < me) & (d >= me - half))
        def _():
            q_copy(me, me, low_send.at[d]).wait_send()

        return carry

    lax.fori_loop(0, n, drain, 0)
    all_num.wait_send()
    all_tot.wait_send()

    @pl.when(far(me, 0))
    def _():
        q_copy(me, me, low_send.at[0]).wait_send()

    @pl.when(me + 1 < n)
    def _():
        q_copy(me, me, up_send).wait_send()

    @pl.when(me == 0)
    def _():
        for w in range(WRAP_PHASES):
            for i in range(WRAP):
                wrap_copy(w, i, me).wait_send()


def body(queries, key_pages, value_pages, page_owner, page_local, seq_lengths):
    n = lax.axis_size("seq")
    per, all_heads, head_dim = queries.shape
    pool, kv, page, _ = key_pages.shape
    heads = all_heads // lax.axis_size("tp")
    rows = per * heads
    seqs, slots = page_owner.shape
    devs = PHASE_ROWS // rows
    assert kv == 1 and pool == LANES and head_dim == LANES and seqs == n * per
    tokens = pool * page
    dma = pltpu.SemaphoreType.DMA
    out = pl.pallas_call(
        functools.partial(kernel, n),
        out_shape=jax.ShapeDtypeStruct((rows, head_dim), jnp.bfloat16),
        in_specs=[pl.BlockSpec(memory_space=pl.ANY)] * 6,
        out_specs=pl.BlockSpec(memory_space=pltpu.VMEM),
        scratch_shapes=[
            pltpu.VMEM(queries.shape, jnp.bfloat16),
            pltpu.VMEM((tokens, head_dim), jnp.bfloat16),
            pltpu.VMEM((tokens, head_dim), jnp.bfloat16),
            pltpu.VMEM((seqs, slots), jnp.int32),
            pltpu.VMEM((seqs, slots), jnp.int32),
            pltpu.SMEM((seqs,), jnp.int32),
            pltpu.VMEM((n, rows, head_dim), jnp.bfloat16),
            pltpu.VMEM((HI, tokens // HI), jnp.float32),
            pltpu.VMEM((n, rows, head_dim), jnp.bfloat16),
            pltpu.VMEM((n // devs, 1, LANES), jnp.float32),
            pltpu.VMEM((n, rows, head_dim), jnp.bfloat16),
            pltpu.VMEM((n, 1, LANES), jnp.float32),
            dma((6,)),
            dma((n,)),
            dma,
            dma((n,)),
            dma((WRAP_PHASES, WRAP)),
            dma((WRAP_PHASES,)),
            dma((n,)),
            dma,
            dma,
            dma,
            dma,
            pltpu.SemaphoreType.REGULAR,
            pltpu.SemaphoreType.REGULAR,
            pltpu.SemaphoreType.REGULAR((WRAP,)),
        ],
        compiler_params=pltpu.CompilerParams(collective_id=0, has_side_effects=True),
        name="paged_attention",
    )(
        queries,
        key_pages.reshape(tokens, head_dim),
        value_pages.reshape(tokens, head_dim),
        page_owner,
        page_local,
        seq_lengths,
    )
    return out.reshape(per, heads, head_dim)


def solution(mesh):
    placed = (
        P(("rep", "seq"), None, None),
        P(("rep", "seq"), "tp", None, None),
        P(("rep", "seq"), "tp", None, None),
        P("rep", None),
        P("rep", None),
        P("rep"),
    )
    return jax.shard_map(
        body, mesh=mesh, in_specs=placed, out_specs=P(("rep", "seq"), "tp", None), check_vma=False
    )
```

```python
import functools
import math

import jax
import jax.numpy as jnp
from jax import lax
from jax.experimental import pallas as pl
from jax.experimental.pallas import tpu as pltpu
from jax.sharding import PartitionSpec as P

SHIFT = 8.0
PHASE_ROWS = 128
LANES = 128
HI = 8
WRAP = 8
WRAP_PHASES = 2
MESH = pl.DeviceIdType.MESH


def kernel(
    n,
    q_hbm,
    k_hbm,
    v_hbm,
    own_hbm,
    loc_hbm,
    len_hbm,
    o_ref,
    q_buf,
    k_buf,
    v_buf,
    own_buf,
    loc_buf,
    len_ref,
    q_all,
    tok_seq,
    num_out,
    tot_out,
    num_in,
    tot_in,
    load_sem,
    low_send,
    up_send,
    up2_send,
    wrap_send,
    wrap_recv,
    q_recv,
    num_send,
    tot_send,
    num_recv,
    tot_recv,
    up_here,
    up2_here,
    wrap_here,
):
    z = lax.axis_index("seq")
    tp = lax.axis_index("tp")
    shift = jnp.where(lax.axis_index("rep") + tp == 0, 1, 0)
    me = lax.rem(z + n - shift, n)

    def at_place(p):
        return {"seq": lax.rem(p + shift, n)}

    per, _, head_dim = q_buf.shape
    heads = q_all.shape[1] // per
    rows = per * heads
    seqs, slots = own_buf.shape
    tokens = k_buf.shape[0]
    chunk = tokens // HI
    page = k_buf.shape[0] // (HI * (LANES // HI))
    lows = LANES // HI
    devs = PHASE_ROWS // rows
    phases = n // devs

    loads = [
        pltpu.make_async_copy(src, dst, load_sem.at[i])
        for i, (src, dst) in enumerate(
            [
                (q_hbm, q_buf),
                (own_hbm, own_buf),
                (loc_hbm, loc_buf),
                (k_hbm, k_buf),
                (v_hbm, v_buf),
                (len_hbm, len_ref),
            ]
        )
    ]
    for load in loads:
        load.start()

    barrier = pltpu.get_barrier_semaphore()

    def greet(d, carry):
        pl.semaphore_signal(barrier, inc=1, device_id=at_place(d), device_id_type=MESH)
        return carry

    lax.fori_loop(me + 1, n, greet, 0)

    @pl.when(me >= 1)
    def _():
        pl.semaphore_wait(barrier, me)
        pl.semaphore_signal(up_here, inc=1, device_id=at_place(me - 1), device_id_type=MESH)

    @pl.when(me >= 2)
    def _():
        pl.semaphore_signal(up2_here, inc=1, device_id=at_place(me - 2), device_id_type=MESH)

    @pl.when(me >= n - WRAP)
    def _():
        pl.semaphore_signal(
            wrap_here.at[me - (n - WRAP)], inc=1, device_id=at_place(0), device_id_type=MESH
        )

    loads[0].wait()
    mine = jnp.zeros((per, heads, head_dim), jnp.float32)
    wide = q_buf[...].astype(jnp.float32)
    for t in range(q_buf.shape[1] // heads):
        mine = jnp.where(tp == t, wide[:, t * heads : (t + 1) * heads, :], mine)
    q_all[me] = mine.reshape(rows, head_dim).astype(jnp.bfloat16)

    def q_copy(j, d, sem):
        return pltpu.make_async_remote_copy(
            src_ref=q_all.at[j],
            dst_ref=q_all.at[j],
            send_sem=sem,
            recv_sem=q_recv.at[j],
            device_id=at_place(d),
            device_id_type=MESH,
        )

    half = n // 2

    def far(j, p):
        return j - p > half

    @pl.when(far(me, 0))
    def _():
        q_copy(me, 0, low_send).start()

    def send_low(d, carry):
        q_copy(me, d, low_send).start()
        return carry

    lax.fori_loop(jnp.maximum(me - half, 0), me, send_low, 0)

    loads[1].wait()
    loads[2].wait()
    loads[5].wait()
    slot = lax.broadcasted_iota(jnp.int32, (8, slots), 1)
    sub = lax.broadcasted_iota(jnp.int32, (8, slots), 0)

    def tally(g, table):
        own = own_buf[pl.ds(pl.multiple_of(g * 8, 8), 8), :]
        loc = loc_buf[pl.ds(pl.multiple_of(g * 8, 8), 8), :]
        length = jnp.zeros((8, slots), jnp.int32)
        for i in range(8):
            length = jnp.where(sub == i, len_ref[g * 8 + i], length)
        fill = jnp.clip(length - slot * page, 0, page)
        key = jnp.where((own == z) & (fill > 0), loc, -1)
        high = key >> (lows.bit_length() - 1)
        low = key & (lows - 1)
        fill_f = fill.astype(jnp.float32)
        seq_f = (g * 8 + sub).astype(jnp.float32)
        left = [jnp.where(high == h, v, 0.0) for v in (seq_f, fill_f) for h in range(HI)]
        right = [jnp.where(low == l, 1.0, 0.0) for l in range(lows)]
        left = jnp.concatenate(left, axis=0).astype(jnp.bfloat16)
        right = jnp.concatenate(right, axis=0).astype(jnp.bfloat16)
        return table + lax.dot_general(
            left, right, (((1,), (1,)), ((), ())), preferred_element_type=jnp.float32
        )

    table = lax.fori_loop(0, seqs // 8, tally, jnp.zeros((2 * HI * 8, lows * 8), jnp.float32))
    row_id = lax.broadcasted_iota(jnp.int32, table.shape, 0)
    col_id = lax.broadcasted_iota(jnp.int32, table.shape, 1)
    table = jnp.where((row_id & 7) == (col_id & 7), table, 0.0).astype(jnp.bfloat16)
    pick = (
        lax.broadcasted_iota(jnp.int32, (2 * HI, 2 * HI * 8), 1) >> 3
        == lax.broadcasted_iota(jnp.int32, (2 * HI, 2 * HI * 8), 0)
    )
    spread = (
        lax.broadcasted_iota(jnp.int32, (lows * 8, chunk), 0) >> 3
        == lax.broadcasted_iota(jnp.int32, (lows * 8, chunk), 1) // page
    )
    pick = jnp.where(pick, 1.0, 0.0).astype(jnp.bfloat16)
    spread = jnp.where(spread, 1.0, 0.0).astype(jnp.bfloat16)
    small = jnp.dot(pick, table, preferred_element_type=jnp.float32).astype(jnp.bfloat16)
    per_token = jnp.dot(small, spread, preferred_element_type=jnp.float32)
    place = (lax.broadcasted_iota(jnp.int32, (HI, chunk), 1) % page).astype(jnp.float32)
    tok_seq[...] = jnp.where(place < per_token[HI:], per_token[:HI], -1.0)

    @pl.when(me + 1 < n)
    def _():
        pl.semaphore_wait(up_here, 1)
        q_copy(me, me + 1, up_send).start()

    @pl.when(me + 2 < n)
    def _():
        pl.semaphore_wait(up2_here, 1)
        q_copy(me, me + 2, up2_send).start()

    def wrap_copy(g, p):
        return pltpu.make_async_remote_copy(
            src_ref=q_all.at[pl.ds(g * devs, devs)],
            dst_ref=q_all.at[pl.ds(g * devs, devs)],
            send_sem=wrap_send,
            recv_sem=wrap_recv.at[g],
            device_id=at_place(p),
            device_id_type=MESH,
        )

    def goes_up(j):
        return ((j < me) & (me + 2 < n) & ((j >= WRAP_PHASES * devs) | (me + 2 < n - WRAP))) | far(
            j, me + 2
        )

    loads[3].wait()
    loads[4].wait()

    def num_copy(d, s):
        return pltpu.make_async_remote_copy(
            src_ref=num_out.at[d],
            dst_ref=num_in.at[s],
            send_sem=num_send,
            recv_sem=num_recv,
            device_id=at_place(d),
            device_id_type=MESH,
        )

    def tot_copy(d, s):
        return pltpu.make_async_remote_copy(
            src_ref=tot_out.at[d // devs],
            dst_ref=tot_in.at[s],
            send_sem=tot_send,
            recv_sem=tot_recv,
            device_id=at_place(d),
            device_id_type=MESH,
        )

    def all_copies(src, dst, send, recv):
        return pltpu.make_async_remote_copy(
            src_ref=src.at[pl.ds(0, n - 1)],
            dst_ref=dst.at[pl.ds(0, n - 1)],
            send_sem=send,
            recv_sem=recv,
            device_id=at_place(me),
            device_id_type=MESH,
        )

    all_num = all_copies(num_in, num_in, num_send, num_recv)
    all_tot = all_copies(tot_in, tot_in, tot_send, tot_recv)

    log2e = math.log2(math.e)
    gain, lift = log2e / math.sqrt(head_dim), SHIFT * log2e
    eye = lax.broadcasted_iota(jnp.int32, (PHASE_ROWS, LANES), 0) == lax.broadcasted_iota(
        jnp.int32, (PHASE_ROWS, LANES), 1
    )

    def phase(g, carry):
        fed = (g < WRAP_PHASES) & (me >= n - WRAP)

        @pl.when(fed)
        def _():
            wrap_copy(g, me).wait_recv()

        def arrived(j, carry):
            @pl.when((j != me) & jnp.logical_not(fed))
            def _():
                q_copy(j, me, up_send).wait_recv()

            @pl.when((me == 0) & far(j, 1))
            def _():
                q_copy(j, 1, low_send).start()

            @pl.when(goes_up(j))
            def _():
                q_copy(j, me + 2, up2_send).start()

            return carry

        start = g * devs
        stop = jnp.where(g < phases // 2, start + devs, jnp.where(g == phases // 2, n, start))
        lax.fori_loop(start, stop, arrived, 0)
        @pl.when((g == WRAP_PHASES - 1) & (me == 0))
        def _():
            for i in range(WRAP):
                pl.semaphore_wait(wrap_here.at[i], 1)
                wrap_copy(0, n - WRAP + i).start()
            for w in range(1, WRAP_PHASES):
                for i in range(WRAP):
                    wrap_copy(w, n - WRAP + i).start()

        q = q_all[pl.ds(g * devs, devs)].reshape(PHASE_ROWS, head_dim)
        row = lax.broadcasted_iota(jnp.int32, (PHASE_ROWS, 1), 0)
        source = g * devs + row // rows + shift
        source = jnp.where(source >= n, source - n, source)
        row_seq = (source * per + row % rows // heads).astype(jnp.float32)

        def tile(c, sums):
            num, tot = sums
            at = pl.ds(pl.multiple_of(c * chunk, chunk), chunk)
            s = lax.dot_general(
                q, k_buf[at, :], (((1,), (1,)), ((), ())), preferred_element_type=jnp.float32
            )
            w = jnp.exp2(s * gain - lift)
            w = jnp.where(tok_seq[pl.ds(c, 1), :] == row_seq, w, 0.0)
            for i in range(chunk // LANES):
                tot = tot + w[:, i * LANES : (i + 1) * LANES]
            num = num + jnp.dot(
                w.astype(jnp.bfloat16), v_buf[at, :], preferred_element_type=jnp.float32
            )
            return num, tot

        zero = jnp.zeros((PHASE_ROWS, LANES), jnp.float32)
        num, tot = lax.fori_loop(0, HI, tile, (zero, zero), unroll=HI)
        num_out[pl.ds(g * devs, devs)] = num.astype(jnp.bfloat16).reshape(devs, rows, head_dim)
        tot = jnp.sum(tot, axis=1, keepdims=True)
        tot_out[g] = jnp.sum(jnp.where(eye, tot, 0.0), axis=0, keepdims=True)

        def give(d, carry):
            @pl.when(d != me)
            def _():
                num_copy(d, me).start()
                tot_copy(d, me).start()

            @pl.when(d == me)
            def _():
                num_in[me] = num_out[me]
                tot_in[me] = tot_out[d // devs]

            return carry

        start = jnp.where(g == 1, devs // 2, g * devs)
        stop = jnp.where(g == 0, devs // 2, (g + 1) * devs)
        lax.fori_loop(start, stop, give, 0)

        return carry

    lax.fori_loop(0, phases, phase, 0)

    def sent(sem, count, most):
        for k in range(1, most + 1):

            @pl.when(count == k)
            def _():
                pltpu.make_async_remote_copy(
                    src_ref=q_all.at[pl.ds(0, k)],
                    dst_ref=q_all.at[pl.ds(0, k)],
                    send_sem=sem,
                    recv_sem=q_recv.at[0],
                    device_id=at_place(me),
                    device_id_type=MESH,
                ).wait_send()

    low = jnp.minimum(me, half) + jnp.where(far(me, 0), 1, 0)
    sent(low_send, jnp.where(me == 0, n - half - 2, low), half + 1)
    below = jnp.where(me + 2 < n - WRAP, me, jnp.maximum(me - WRAP_PHASES * devs, 0))
    up2 = jnp.where(me + 2 < n, below + 1, 0) + jnp.maximum(n - 3 - me - half, 0)
    sent(up2_send, up2, n)

    @pl.when(me + 1 < n)
    def _():
        q_copy(me, me, up_send).wait_send()

    @pl.when(me == 0)
    def _():
        fed_rows = WRAP_PHASES * WRAP * devs * rows
        pltpu.make_async_remote_copy(
            src_ref=k_buf.at[pl.ds(0, fed_rows)],
            dst_ref=k_buf.at[pl.ds(0, fed_rows)],
            send_sem=wrap_send,
            recv_sem=q_recv.at[0],
            device_id=at_place(me),
            device_id_type=MESH,
        ).wait_send()

    all_num.wait_recv()
    all_tot.wait_recv()
    num = jnp.sum(num_in[...].astype(jnp.float32), axis=0)
    tot = jnp.sum(tot_in[...], axis=0)
    at = lax.broadcasted_iota(jnp.int32, (rows, LANES), 0) + lax.rem(me, devs) * rows
    tot = jnp.where(lax.broadcasted_iota(jnp.int32, (rows, LANES), 1) == at, tot, 0.0)
    o_ref[...] = (num / jnp.sum(tot, axis=1, keepdims=True)).astype(jnp.bfloat16)
    all_num.wait_send()
    all_tot.wait_send()


def body(queries, key_pages, value_pages, page_owner, page_local, seq_lengths):
    n = lax.axis_size("seq")
    per, all_heads, head_dim = queries.shape
    pool, kv, page, _ = key_pages.shape
    heads = all_heads // lax.axis_size("tp")
    rows = per * heads
    seqs, slots = page_owner.shape
    devs = PHASE_ROWS // rows
    assert kv == 1 and pool == LANES and head_dim == LANES and seqs == n * per
    tokens = pool * page
    dma = pltpu.SemaphoreType.DMA
    out = pl.pallas_call(
        functools.partial(kernel, n),
        out_shape=pltpu.VMEM((rows, head_dim), jnp.bfloat16),
        in_specs=[pl.BlockSpec(memory_space=pl.ANY)] * 6,
        out_specs=pl.BlockSpec(memory_space=pltpu.VMEM),
        scratch_shapes=[
            pltpu.VMEM(queries.shape, jnp.bfloat16),
            pltpu.VMEM((tokens, head_dim), jnp.bfloat16),
            pltpu.VMEM((tokens, head_dim), jnp.bfloat16),
            pltpu.VMEM((seqs, slots), jnp.int32),
            pltpu.VMEM((seqs, slots), jnp.int32),
            pltpu.SMEM((seqs,), jnp.int32),
            pltpu.VMEM((n, rows, head_dim), jnp.bfloat16),
            pltpu.VMEM((HI, tokens // HI), jnp.float32),
            pltpu.VMEM((n, rows, head_dim), jnp.bfloat16),
            pltpu.VMEM((n // devs, 1, LANES), jnp.float32),
            pltpu.VMEM((n, rows, head_dim), jnp.bfloat16),
            pltpu.VMEM((n, 1, LANES), jnp.float32),
            dma((6,)),
            dma,
            dma,
            dma,
            dma,
            dma((WRAP_PHASES,)),
            dma((n,)),
            dma,
            dma,
            dma,
            dma,
            pltpu.SemaphoreType.REGULAR,
            pltpu.SemaphoreType.REGULAR,
            pltpu.SemaphoreType.REGULAR((WRAP,)),
        ],
        compiler_params=pltpu.CompilerParams(collective_id=0, has_side_effects=True),
        name="paged_attention",
    )(
        queries,
        key_pages.reshape(tokens, head_dim),
        value_pages.reshape(tokens, head_dim),
        page_owner,
        page_local,
        seq_lengths,
    )
    return out.reshape(per, heads, head_dim)


def solution(mesh):
    placed = (
        P(("rep", "seq"), None, None),
        P(("rep", "seq"), "tp", None, None),
        P(("rep", "seq"), "tp", None, None),
        P("rep", None),
        P("rep", None),
        P("rep"),
    )
    return jax.shard_map(
        body, mesh=mesh, in_specs=placed, out_specs=P(("rep", "seq"), "tp", None), check_vma=False
    )
```

```python
import functools
import math

import jax
import jax.numpy as jnp
from jax import lax
from jax.experimental import pallas as pl
from jax.experimental.pallas import tpu as pltpu
from jax.sharding import PartitionSpec as P

SHIFT = 8.0
PHASE_ROWS = 128
LANES = 128
HI = 8
WRAP = 6
HOP = 4
WRAP_PHASES = 2
MESH = pl.DeviceIdType.MESH


def kernel(
    n,
    q_hbm,
    k_hbm,
    v_hbm,
    own_hbm,
    loc_hbm,
    len_hbm,
    o_ref,
    q_buf,
    k_buf,
    v_buf,
    own_buf,
    loc_buf,
    len_ref,
    q_all,
    tok_seq,
    num_out,
    tot_out,
    num_in,
    tot_in,
    load_sem,
    low_send,
    up_send,
    up2_send,
    hop_send,
    wrap_send,
    wrap_recv,
    q_recv,
    num_send,
    tot_send,
    num_recv,
    tot_recv,
    up_here,
    up2_here,
    hop_here,
    wrap_here,
):
    z = lax.axis_index("seq")
    tp = lax.axis_index("tp")
    shift = jnp.where(lax.axis_index("rep") + tp == 0, 1, 0)
    me = lax.rem(z + n - shift, n)

    def at_place(p):
        return {"seq": lax.rem(p + shift, n)}

    per, _, head_dim = q_buf.shape
    heads = q_all.shape[1] // per
    rows = per * heads
    seqs, slots = own_buf.shape
    tokens = k_buf.shape[0]
    chunk = tokens // HI
    page = k_buf.shape[0] // (HI * (LANES // HI))
    lows = LANES // HI
    devs = PHASE_ROWS // rows
    phases = n // devs

    loads = [
        pltpu.make_async_copy(src, dst, load_sem.at[i])
        for i, (src, dst) in enumerate(
            [
                (q_hbm, q_buf),
                (own_hbm, own_buf),
                (loc_hbm, loc_buf),
                (k_hbm, k_buf),
                (v_hbm, v_buf),
                (len_hbm, len_ref),
            ]
        )
    ]
    for load in loads:
        load.start()

    barrier = pltpu.get_barrier_semaphore()

    def greet(d, carry):
        pl.semaphore_signal(barrier, inc=1, device_id=at_place(d), device_id_type=MESH)
        return carry

    lax.fori_loop(me + 1, n, greet, 0)

    @pl.when(me >= 1)
    def _():
        pl.semaphore_wait(barrier, me)
        pl.semaphore_signal(up_here, inc=1, device_id=at_place(me - 1), device_id_type=MESH)

    @pl.when(me >= 2)
    def _():
        pl.semaphore_signal(up2_here, inc=1, device_id=at_place(me - 2), device_id_type=MESH)

    half = n // 2
    first_hop = min(half + HOP, n - WRAP)

    @pl.when((me >= first_hop) & (me < n - WRAP))
    def _():
        pl.semaphore_signal(hop_here, inc=1, device_id=at_place(me - HOP), device_id_type=MESH)

    @pl.when(me >= n - WRAP)
    def _():
        pl.semaphore_signal(
            wrap_here.at[me - (n - WRAP)], inc=1, device_id=at_place(0), device_id_type=MESH
        )

    loads[0].wait()
    mine = jnp.zeros((per, heads, head_dim), jnp.float32)
    wide = q_buf[...].astype(jnp.float32)
    for t in range(q_buf.shape[1] // heads):
        mine = jnp.where(tp == t, wide[:, t * heads : (t + 1) * heads, :], mine)
    q_all[me] = mine.reshape(rows, head_dim).astype(jnp.bfloat16)

    def q_copy(j, d, sem):
        return pltpu.make_async_remote_copy(
            src_ref=q_all.at[j],
            dst_ref=q_all.at[j],
            send_sem=sem,
            recv_sem=q_recv.at[j],
            device_id=at_place(d),
            device_id_type=MESH,
        )

    def far(j, p):
        return j - p > half

    @pl.when(far(me, 0))
    def _():
        q_copy(me, 0, low_send).start()

    def send_low(d, carry):
        q_copy(me, d, low_send).start()
        return carry

    lax.fori_loop(jnp.maximum(me - half, 0), me, send_low, 0)

    loads[1].wait()
    loads[2].wait()
    loads[5].wait()
    slot = lax.broadcasted_iota(jnp.int32, (8, slots), 1)
    sub = lax.broadcasted_iota(jnp.int32, (8, slots), 0)

    def tally(g, table):
        own = own_buf[pl.ds(pl.multiple_of(g * 8, 8), 8), :]
        loc = loc_buf[pl.ds(pl.multiple_of(g * 8, 8), 8), :]
        length = jnp.zeros((8, slots), jnp.int32)
        for i in range(8):
            length = jnp.where(sub == i, len_ref[g * 8 + i], length)
        fill = jnp.clip(length - slot * page, 0, page)
        key = jnp.where((own == z) & (fill > 0), loc, -1)
        high = key >> (lows.bit_length() - 1)
        low = key & (lows - 1)
        fill_f = fill.astype(jnp.float32)
        seq_f = (g * 8 + sub).astype(jnp.float32)
        left = [jnp.where(high == h, v, 0.0) for v in (seq_f, fill_f) for h in range(HI)]
        right = [jnp.where(low == l, 1.0, 0.0) for l in range(lows)]
        left = jnp.concatenate(left, axis=0).astype(jnp.bfloat16)
        right = jnp.concatenate(right, axis=0).astype(jnp.bfloat16)
        return table + lax.dot_general(
            left, right, (((1,), (1,)), ((), ())), preferred_element_type=jnp.float32
        )

    table = lax.fori_loop(0, seqs // 8, tally, jnp.zeros((2 * HI * 8, lows * 8), jnp.float32))
    row_id = lax.broadcasted_iota(jnp.int32, table.shape, 0)
    col_id = lax.broadcasted_iota(jnp.int32, table.shape, 1)
    table = jnp.where((row_id & 7) == (col_id & 7), table, 0.0).astype(jnp.bfloat16)
    pick = (
        lax.broadcasted_iota(jnp.int32, (2 * HI, 2 * HI * 8), 1) >> 3
        == lax.broadcasted_iota(jnp.int32, (2 * HI, 2 * HI * 8), 0)
    )
    spread = (
        lax.broadcasted_iota(jnp.int32, (lows * 8, chunk), 0) >> 3
        == lax.broadcasted_iota(jnp.int32, (lows * 8, chunk), 1) // page
    )
    pick = jnp.where(pick, 1.0, 0.0).astype(jnp.bfloat16)
    spread = jnp.where(spread, 1.0, 0.0).astype(jnp.bfloat16)
    small = jnp.dot(pick, table, preferred_element_type=jnp.float32).astype(jnp.bfloat16)
    per_token = jnp.dot(small, spread, preferred_element_type=jnp.float32)
    place = (lax.broadcasted_iota(jnp.int32, (HI, chunk), 1) % page).astype(jnp.float32)
    tok_seq[...] = jnp.where(place < per_token[HI:], per_token[:HI], -1.0)

    @pl.when(me + 1 < n)
    def _():
        pl.semaphore_wait(up_here, 1)
        q_copy(me, me + 1, up_send).start()

    @pl.when(me + 2 < n)
    def _():
        pl.semaphore_wait(up2_here, 1)
        q_copy(me, me + 2, up2_send).start()

    def wrap_copy(g, p):
        return pltpu.make_async_remote_copy(
            src_ref=q_all.at[pl.ds(g * devs, devs)],
            dst_ref=q_all.at[pl.ds(g * devs, devs)],
            send_sem=wrap_send,
            recv_sem=wrap_recv.at[g],
            device_id=at_place(p),
            device_id_type=MESH,
        )

    def hop_copy(p):
        return pltpu.make_async_remote_copy(
            src_ref=q_all.at[pl.ds(0, devs)],
            dst_ref=q_all.at[pl.ds(0, devs)],
            send_sem=hop_send,
            recv_sem=wrap_recv.at[0],
            device_id=at_place(p),
            device_id_type=MESH,
        )

    def goes_up(j):
        limit = jnp.where(j < devs, first_hop, jnp.where(j < WRAP_PHASES * devs, n - WRAP, n))
        return ((j < me) & (me + 2 < limit)) | far(j, me + 2)

    hops = (me + HOP >= first_hop) & (me + HOP < n - WRAP)

    loads[3].wait()
    loads[4].wait()

    def num_copy(d, s):
        return pltpu.make_async_remote_copy(
            src_ref=num_out.at[d],
            dst_ref=num_in.at[s],
            send_sem=num_send,
            recv_sem=num_recv,
            device_id=at_place(d),
            device_id_type=MESH,
        )

    def tot_copy(d, s):
        return pltpu.make_async_remote_copy(
            src_ref=tot_out.at[d // devs],
            dst_ref=tot_in.at[s],
            send_sem=tot_send,
            recv_sem=tot_recv,
            device_id=at_place(d),
            device_id_type=MESH,
        )

    def all_copies(src, dst, send, recv):
        return pltpu.make_async_remote_copy(
            src_ref=src.at[pl.ds(0, n - 1)],
            dst_ref=dst.at[pl.ds(0, n - 1)],
            send_sem=send,
            recv_sem=recv,
            device_id=at_place(me),
            device_id_type=MESH,
        )

    all_num = all_copies(num_in, num_in, num_send, num_recv)
    all_tot = all_copies(tot_in, tot_in, tot_send, tot_recv)

    log2e = math.log2(math.e)
    gain, lift = log2e / math.sqrt(head_dim), SHIFT * log2e
    eye = lax.broadcasted_iota(jnp.int32, (PHASE_ROWS, LANES), 0) == lax.broadcasted_iota(
        jnp.int32, (PHASE_ROWS, LANES), 1
    )

    def give(d, carry):
        @pl.when(d != me)
        def _():
            num_copy(d, me).start()
            tot_copy(d, me).start()

        @pl.when(d == me)
        def _():
            num_in[me] = num_out[me]
            tot_in[me] = tot_out[d // devs]

        return carry

    def phase(g, carry):
        fed = ((g == 0) & (me >= first_hop)) | ((g < WRAP_PHASES) & (me >= n - WRAP))

        @pl.when(fed)
        def _():
            wrap_copy(g, me).wait_recv()

        def arrived(j, carry):
            @pl.when((j != me) & jnp.logical_not(fed))
            def _():
                q_copy(j, me, up_send).wait_recv()

            @pl.when((me == 0) & far(j, 1))
            def _():
                q_copy(j, 1, low_send).start()

            @pl.when(goes_up(j))
            def _():
                q_copy(j, me + 2, up2_send).start()

            return carry

        start = g * devs
        stop = jnp.where(g < phases // 2, start + devs, jnp.where(g == phases // 2, n, start))
        lax.fori_loop(start, stop, arrived, 0)
        @pl.when((g == 0) & hops)
        def _():
            pl.semaphore_wait(hop_here, 1)
            hop_copy(me + HOP).start()

        @pl.when((g == WRAP_PHASES - 1) & (me == 0))
        def _():
            for i in range(WRAP):
                pl.semaphore_wait(wrap_here.at[i], 1)
                wrap_copy(0, n - WRAP + i).start()
            for w in range(1, WRAP_PHASES):
                for i in range(WRAP):
                    wrap_copy(w, n - WRAP + i).start()

        @pl.when(g == 1)
        def _():
            lax.fori_loop(devs // 2, devs, give, 0)

        q = q_all[pl.ds(g * devs, devs)].reshape(PHASE_ROWS, head_dim)
        row = lax.broadcasted_iota(jnp.int32, (PHASE_ROWS, 1), 0)
        source = g * devs + row // rows + shift
        source = jnp.where(source >= n, source - n, source)
        row_seq = (source * per + row % rows // heads).astype(jnp.float32)

        def tile(c, sums):
            num, tot = sums
            at = pl.ds(pl.multiple_of(c * chunk, chunk), chunk)
            s = lax.dot_general(
                q, k_buf[at, :], (((1,), (1,)), ((), ())), preferred_element_type=jnp.float32
            )
            w = jnp.exp2(s * gain - lift)
            w = jnp.where(tok_seq[pl.ds(c, 1), :] == row_seq, w, 0.0)
            for i in range(chunk // LANES):
                tot = tot + w[:, i * LANES : (i + 1) * LANES]
            num = num + jnp.dot(
                w.astype(jnp.bfloat16), v_buf[at, :], preferred_element_type=jnp.float32
            )
            return num, tot

        zero = jnp.zeros((PHASE_ROWS, LANES), jnp.float32)
        num, tot = lax.fori_loop(0, HI, tile, (zero, zero), unroll=HI)
        num_out[pl.ds(g * devs, devs)] = num.astype(jnp.bfloat16).reshape(devs, rows, head_dim)
        tot = jnp.sum(tot, axis=1, keepdims=True)
        tot_out[g] = jnp.sum(jnp.where(eye, tot, 0.0), axis=0, keepdims=True)

        stop = jnp.where(g == 0, devs // 2, (g + 1) * devs)
        lax.fori_loop(g * devs, stop, give, 0)
        return carry

    lax.fori_loop(0, phases, phase, 0)

    def sent(sem, count, most):
        for k in range(1, most + 1):

            @pl.when(count == k)
            def _():
                pltpu.make_async_remote_copy(
                    src_ref=q_all.at[pl.ds(0, k)],
                    dst_ref=q_all.at[pl.ds(0, k)],
                    send_sem=sem,
                    recv_sem=q_recv.at[0],
                    device_id=at_place(me),
                    device_id_type=MESH,
                ).wait_send()

    low = jnp.minimum(me, half) + jnp.where(far(me, 0), 1, 0)
    sent(low_send, jnp.where(me == 0, n - half - 2, low), half + 1)
    below = jnp.where(me + 2 < n - WRAP, me - devs, jnp.maximum(me - WRAP_PHASES * devs, 0))
    below = jnp.where(me + 2 < first_hop, me, below)
    up2 = jnp.where(me + 2 < n, below + 1, 0) + jnp.maximum(n - 3 - me - half, 0)
    sent(up2_send, up2, n)

    @pl.when(me + 1 < n)
    def _():
        q_copy(me, me, up_send).wait_send()

    @pl.when(hops)
    def _():
        hop_copy(me).wait_send()

    @pl.when(me == 0)
    def _():
        fed_rows = WRAP_PHASES * WRAP * devs * rows
        pltpu.make_async_remote_copy(
            src_ref=k_buf.at[pl.ds(0, fed_rows)],
            dst_ref=k_buf.at[pl.ds(0, fed_rows)],
            send_sem=wrap_send,
            recv_sem=q_recv.at[0],
            device_id=at_place(me),
            device_id_type=MESH,
        ).wait_send()

    all_num.wait_recv()
    all_tot.wait_recv()
    num = jnp.sum(num_in[...].astype(jnp.float32), axis=0)
    tot = jnp.sum(tot_in[...], axis=0)
    at = lax.broadcasted_iota(jnp.int32, (rows, LANES), 0) + lax.rem(me, devs) * rows
    tot = jnp.where(lax.broadcasted_iota(jnp.int32, (rows, LANES), 1) == at, tot, 0.0)
    o_ref[...] = (num / jnp.sum(tot, axis=1, keepdims=True)).astype(jnp.bfloat16)
    all_num.wait_send()
    all_tot.wait_send()


def body(queries, key_pages, value_pages, page_owner, page_local, seq_lengths):
    n = lax.axis_size("seq")
    per, all_heads, head_dim = queries.shape
    pool, kv, page, _ = key_pages.shape
    heads = all_heads // lax.axis_size("tp")
    rows = per * heads
    seqs, slots = page_owner.shape
    devs = PHASE_ROWS // rows
    assert kv == 1 and pool == LANES and head_dim == LANES and seqs == n * per
    tokens = pool * page
    dma = pltpu.SemaphoreType.DMA
    out = pl.pallas_call(
        functools.partial(kernel, n),
        out_shape=pltpu.VMEM((rows, head_dim), jnp.bfloat16),
        in_specs=[pl.BlockSpec(memory_space=pl.ANY)] * 6,
        out_specs=pl.BlockSpec(memory_space=pltpu.VMEM),
        scratch_shapes=[
            pltpu.VMEM(queries.shape, jnp.bfloat16),
            pltpu.VMEM((tokens, head_dim), jnp.bfloat16),
            pltpu.VMEM((tokens, head_dim), jnp.bfloat16),
            pltpu.VMEM((seqs, slots), jnp.int32),
            pltpu.VMEM((seqs, slots), jnp.int32),
            pltpu.SMEM((seqs,), jnp.int32),
            pltpu.VMEM((n, rows, head_dim), jnp.bfloat16),
            pltpu.VMEM((HI, tokens // HI), jnp.float32),
            pltpu.VMEM((n, rows, head_dim), jnp.bfloat16),
            pltpu.VMEM((n // devs, 1, LANES), jnp.float32),
            pltpu.VMEM((n, rows, head_dim), jnp.bfloat16),
            pltpu.VMEM((n, 1, LANES), jnp.float32),
            dma((6,)),
            dma,
            dma,
            dma,
            dma,
            dma,
            dma((WRAP_PHASES,)),
            dma((n,)),
            dma,
            dma,
            dma,
            dma,
            pltpu.SemaphoreType.REGULAR,
            pltpu.SemaphoreType.REGULAR,
            pltpu.SemaphoreType.REGULAR,
            pltpu.SemaphoreType.REGULAR((WRAP,)),
        ],
        compiler_params=pltpu.CompilerParams(collective_id=0, has_side_effects=True),
        name="paged_attention",
    )(
        queries,
        key_pages.reshape(tokens, head_dim),
        value_pages.reshape(tokens, head_dim),
        page_owner,
        page_local,
        seq_lengths,
    )
    return out.reshape(per, heads, head_dim)


def solution(mesh):
    placed = (
        P(("rep", "seq"), None, None),
        P(("rep", "seq"), "tp", None, None),
        P(("rep", "seq"), "tp", None, None),
        P("rep", None),
        P("rep", None),
        P("rep"),
    )
    return jax.shard_map(
        body, mesh=mesh, in_specs=placed, out_specs=P(("rep", "seq"), "tp", None), check_vma=False
    )
```

```python
import functools
import math

import jax
import jax.numpy as jnp
from jax import lax
from jax.experimental import pallas as pl
from jax.experimental.pallas import tpu as pltpu
from jax.sharding import PartitionSpec as P

SHIFT = 8.0
PHASE_ROWS = 128
LANES = 128
HI = 8
WRAP = 6
HOP = 4
WRAP_PHASES = 2
MESH = pl.DeviceIdType.MESH


def kernel(
    n,
    q_hbm,
    k_hbm,
    v_hbm,
    own_hbm,
    loc_hbm,
    len_hbm,
    o_ref,
    q_buf,
    k_buf,
    v_buf,
    own_buf,
    loc_buf,
    len_ref,
    q_all,
    tok_seq,
    num_out,
    tot_out,
    num_in,
    tot_in,
    load_sem,
    low_send,
    up_send,
    up2_send,
    hop_send,
    wrap_send,
    wrap_recv,
    q_recv,
    num_send,
    tot_send,
    num_recv,
    tot_recv,
    up_here,
    up2_here,
    hop_here,
    wrap_here,
):
    z = lax.axis_index("seq")
    tp = lax.axis_index("tp")
    shift = jnp.where(lax.axis_index("rep") + tp == 0, 1, 0)
    me = lax.rem(z + n - shift, n)

    def at_place(p):
        return {"seq": lax.rem(p + shift, n)}

    per, _, head_dim = q_buf.shape
    heads = q_all.shape[1] // per
    rows = per * heads
    seqs, slots = own_buf.shape
    tokens = k_buf.shape[0]
    chunk = tokens // HI
    page = k_buf.shape[0] // (HI * (LANES // HI))
    lows = LANES // HI
    devs = PHASE_ROWS // rows
    phases = n // devs

    loads = [
        pltpu.make_async_copy(src, dst, load_sem.at[i])
        for i, (src, dst) in enumerate(
            [
                (q_hbm, q_buf),
                (own_hbm, own_buf),
                (loc_hbm, loc_buf),
                (k_hbm, k_buf),
                (v_hbm, v_buf),
                (len_hbm, len_ref),
            ]
        )
    ]
    for load in loads:
        load.start()

    barrier = pltpu.get_barrier_semaphore()

    def greet(d, carry):
        pl.semaphore_signal(barrier, inc=1, device_id=at_place(d), device_id_type=MESH)
        return carry

    lax.fori_loop(me + 1, n, greet, 0)

    @pl.when(me >= 1)
    def _():
        pl.semaphore_wait(barrier, me)
        pl.semaphore_signal(up_here, inc=1, device_id=at_place(me - 1), device_id_type=MESH)

    @pl.when(me >= 2)
    def _():
        pl.semaphore_signal(up2_here, inc=1, device_id=at_place(me - 2), device_id_type=MESH)

    half = n // 2
    first_hop = min(half + HOP, n - WRAP)

    @pl.when((me >= first_hop) & (me < n - WRAP))
    def _():
        pl.semaphore_signal(hop_here, inc=1, device_id=at_place(me - HOP), device_id_type=MESH)

    @pl.when(me >= n - WRAP)
    def _():
        pl.semaphore_signal(
            wrap_here.at[me - (n - WRAP)], inc=1, device_id=at_place(0), device_id_type=MESH
        )

    loads[0].wait()
    mine = jnp.zeros((per, heads, head_dim), jnp.float32)
    wide = q_buf[...].astype(jnp.float32)
    for t in range(q_buf.shape[1] // heads):
        mine = jnp.where(tp == t, wide[:, t * heads : (t + 1) * heads, :], mine)
    q_all[me] = mine.reshape(rows, head_dim).astype(jnp.bfloat16)

    def q_copy(j, d, sem):
        return pltpu.make_async_remote_copy(
            src_ref=q_all.at[j],
            dst_ref=q_all.at[j],
            send_sem=sem,
            recv_sem=q_recv.at[j],
            device_id=at_place(d),
            device_id_type=MESH,
        )

    def far(j, p):
        return j - p > half

    @pl.when(far(me, 0))
    def _():
        q_copy(me, 0, low_send).start()

    def send_low(d, carry):
        q_copy(me, d, low_send).start()
        return carry

    lax.fori_loop(jnp.maximum(me - half, 0), me, send_low, 0)

    loads[1].wait()
    loads[2].wait()
    loads[5].wait()
    slot = lax.broadcasted_iota(jnp.int32, (8, slots), 1)
    sub = lax.broadcasted_iota(jnp.int32, (8, slots), 0)

    def tally(g, table):
        own = own_buf[pl.ds(pl.multiple_of(g * 8, 8), 8), :]
        loc = loc_buf[pl.ds(pl.multiple_of(g * 8, 8), 8), :]
        length = jnp.zeros((8, slots), jnp.int32)
        for i in range(8):
            length = jnp.where(sub == i, len_ref[g * 8 + i], length)
        fill = jnp.clip(length - slot * page, 0, page)
        key = jnp.where((own == z) & (fill > 0), loc, -1)
        high = key >> (lows.bit_length() - 1)
        low = key & (lows - 1)
        fill_f = fill.astype(jnp.float32)
        seq_f = (g * 8 + sub).astype(jnp.float32)
        left = [jnp.where(high == h, v, 0.0) for v in (seq_f, fill_f) for h in range(HI)]
        right = [jnp.where(low == l, 1.0, 0.0) for l in range(lows)]
        left = jnp.concatenate(left, axis=0).astype(jnp.bfloat16)
        right = jnp.concatenate(right, axis=0).astype(jnp.bfloat16)
        return table + lax.dot_general(
            left, right, (((1,), (1,)), ((), ())), preferred_element_type=jnp.float32
        )

    table = lax.fori_loop(0, seqs // 8, tally, jnp.zeros((2 * HI * 8, lows * 8), jnp.float32))
    row_id = lax.broadcasted_iota(jnp.int32, table.shape, 0)
    col_id = lax.broadcasted_iota(jnp.int32, table.shape, 1)
    table = jnp.where((row_id & 7) == (col_id & 7), table, 0.0).astype(jnp.bfloat16)
    pick = (
        lax.broadcasted_iota(jnp.int32, (2 * HI, 2 * HI * 8), 1) >> 3
        == lax.broadcasted_iota(jnp.int32, (2 * HI, 2 * HI * 8), 0)
    )
    spread = (
        lax.broadcasted_iota(jnp.int32, (lows * 8, chunk), 0) >> 3
        == lax.broadcasted_iota(jnp.int32, (lows * 8, chunk), 1) // page
    )
    pick = jnp.where(pick, 1.0, 0.0).astype(jnp.bfloat16)
    spread = jnp.where(spread, 1.0, 0.0).astype(jnp.bfloat16)
    small = jnp.dot(pick, table, preferred_element_type=jnp.float32).astype(jnp.bfloat16)
    per_token = jnp.dot(small, spread, preferred_element_type=jnp.float32)
    place = (lax.broadcasted_iota(jnp.int32, (HI, chunk), 1) % page).astype(jnp.float32)
    tok_seq[...] = jnp.where(place < per_token[HI:], per_token[:HI], -1.0)

    @pl.when(me + 1 < n)
    def _():
        pl.semaphore_wait(up_here, 1)
        q_copy(me, me + 1, up_send).start()

    @pl.when(me + 2 < n)
    def _():
        pl.semaphore_wait(up2_here, 1)
        q_copy(me, me + 2, up2_send).start()

    def wrap_copy(g, p):
        return pltpu.make_async_remote_copy(
            src_ref=q_all.at[pl.ds(g * devs, devs)],
            dst_ref=q_all.at[pl.ds(g * devs, devs)],
            send_sem=wrap_send,
            recv_sem=wrap_recv.at[g],
            device_id=at_place(p),
            device_id_type=MESH,
        )

    def hop_copy(p):
        return pltpu.make_async_remote_copy(
            src_ref=q_all.at[pl.ds(0, devs)],
            dst_ref=q_all.at[pl.ds(0, devs)],
            send_sem=hop_send,
            recv_sem=wrap_recv.at[0],
            device_id=at_place(p),
            device_id_type=MESH,
        )

    def goes_up(j):
        limit = jnp.where(j < devs, first_hop, jnp.where(j < WRAP_PHASES * devs, n - WRAP, n))
        return ((j < me) & (me + 2 < limit)) | far(j, me + 2)

    hops = (me + HOP >= first_hop) & (me + HOP < n - WRAP)

    loads[3].wait()
    loads[4].wait()

    def num_copy(d, s):
        return pltpu.make_async_remote_copy(
            src_ref=num_out.at[d],
            dst_ref=num_in.at[s],
            send_sem=num_send,
            recv_sem=num_recv,
            device_id=at_place(d),
            device_id_type=MESH,
        )

    def tot_copy(d, s):
        return pltpu.make_async_remote_copy(
            src_ref=tot_out.at[d // devs],
            dst_ref=tot_in.at[s],
            send_sem=tot_send,
            recv_sem=tot_recv,
            device_id=at_place(d),
            device_id_type=MESH,
        )

    def all_copies(src, dst, send, recv):
        return pltpu.make_async_remote_copy(
            src_ref=src.at[pl.ds(0, n - 1)],
            dst_ref=dst.at[pl.ds(0, n - 1)],
            send_sem=send,
            recv_sem=recv,
            device_id=at_place(me),
            device_id_type=MESH,
        )

    all_num = all_copies(num_in, num_in, num_send, num_recv)
    all_tot = all_copies(tot_in, tot_in, tot_send, tot_recv)

    log2e = math.log2(math.e)
    gain, lift = log2e / math.sqrt(head_dim), SHIFT * log2e
    eye = lax.broadcasted_iota(jnp.int32, (PHASE_ROWS, LANES), 0) == lax.broadcasted_iota(
        jnp.int32, (PHASE_ROWS, LANES), 1
    )

    def give(d, carry):
        @pl.when(d != me)
        def _():
            num_copy(d, me).start()
            tot_copy(d, me).start()

        @pl.when(d == me)
        def _():
            num_in[me] = num_out[me]
            tot_in[me] = tot_out[d // devs]

        return carry

    def phase(g, carry):
        fed = ((g == 0) & (me >= first_hop)) | ((g < WRAP_PHASES) & (me >= n - WRAP))

        @pl.when(fed)
        def _():
            wrap_copy(g, me).wait_recv()

        def arrived(j, carry):
            @pl.when((j != me) & jnp.logical_not(fed))
            def _():
                q_copy(j, me, up_send).wait_recv()

            @pl.when((me == 0) & far(j, 1))
            def _():
                q_copy(j, 1, low_send).start()

            @pl.when(goes_up(j))
            def _():
                q_copy(j, me + 2, up2_send).start()

            return carry

        start = g * devs
        stop = jnp.where(g < phases // 2, start + devs, jnp.where(g == phases // 2, n, start))
        lax.fori_loop(start, stop, arrived, 0)
        @pl.when((g == 0) & hops)
        def _():
            pl.semaphore_wait(hop_here, 1)
            hop_copy(me + HOP).start()

        @pl.when((g == WRAP_PHASES - 1) & (me == 0))
        def _():
            for i in range(WRAP):
                pl.semaphore_wait(wrap_here.at[i], 1)
                wrap_copy(0, n - WRAP + i).start()
            for w in range(1, WRAP_PHASES):
                for i in range(WRAP):
                    wrap_copy(w, n - WRAP + i).start()

        q = q_all[pl.ds(g * devs, devs)].reshape(PHASE_ROWS, head_dim)
        row = lax.broadcasted_iota(jnp.int32, (PHASE_ROWS, 1), 0)
        source = g * devs + row // rows + shift
        source = jnp.where(source >= n, source - n, source)
        row_seq = (source * per + row % rows // heads).astype(jnp.float32)

        def tile(c, sums):
            num, tot = sums
            at = pl.ds(pl.multiple_of(c * chunk, chunk), chunk)
            s = lax.dot_general(
                q, k_buf[at, :], (((1,), (1,)), ((), ())), preferred_element_type=jnp.float32
            )
            w = jnp.exp2(s * gain - lift)
            w = jnp.where(tok_seq[pl.ds(c, 1), :] == row_seq, w, 0.0)
            for i in range(chunk // LANES):
                tot = tot + w[:, i * LANES : (i + 1) * LANES]
            num = num + jnp.dot(
                w.astype(jnp.bfloat16), v_buf[at, :], preferred_element_type=jnp.float32
            )
            return num, tot

        zero = jnp.zeros((PHASE_ROWS, LANES), jnp.float32)
        num, tot = lax.fori_loop(0, HI, tile, (zero, zero), unroll=HI)
        num_out[pl.ds(g * devs, devs)] = num.astype(jnp.bfloat16).reshape(devs, rows, head_dim)
        tot = jnp.sum(tot, axis=1, keepdims=True)
        tot_out[g] = jnp.sum(jnp.where(eye, tot, 0.0), axis=0, keepdims=True)

        start = jnp.where(g == 1, devs // 2, g * devs)
        stop = jnp.where(g == 0, devs // 2, (g + 1) * devs)
        lax.fori_loop(start, stop, give, 0)
        return carry

    lax.fori_loop(0, phases, phase, 0)

    def sent(sem, count, most):
        for k in range(1, most + 1):

            @pl.when(count == k)
            def _():
                pltpu.make_async_remote_copy(
                    src_ref=q_all.at[pl.ds(0, k)],
                    dst_ref=q_all.at[pl.ds(0, k)],
                    send_sem=sem,
                    recv_sem=q_recv.at[0],
                    device_id=at_place(me),
                    device_id_type=MESH,
                ).wait_send()

    low = jnp.minimum(me, half) + jnp.where(far(me, 0), 1, 0)
    sent(low_send, jnp.where(me == 0, n - half - 2, low), half + 1)
    below = jnp.where(me + 2 < n - WRAP, me - devs, jnp.maximum(me - WRAP_PHASES * devs, 0))
    below = jnp.where(me + 2 < first_hop, me, below)
    up2 = jnp.where(me + 2 < n, below + 1, 0) + jnp.maximum(n - 3 - me - half, 0)
    sent(up2_send, up2, n)

    @pl.when(me + 1 < n)
    def _():
        q_copy(me, me, up_send).wait_send()

    @pl.when(hops)
    def _():
        hop_copy(me).wait_send()

    @pl.when(me == 0)
    def _():
        fed_rows = WRAP_PHASES * WRAP * devs * rows
        pltpu.make_async_remote_copy(
            src_ref=k_buf.at[pl.ds(0, fed_rows)],
            dst_ref=k_buf.at[pl.ds(0, fed_rows)],
            send_sem=wrap_send,
            recv_sem=q_recv.at[0],
            device_id=at_place(me),
            device_id_type=MESH,
        ).wait_send()

    all_num.wait_recv()
    all_tot.wait_recv()
    num = jnp.sum(num_in[...].astype(jnp.float32), axis=0)
    tot = jnp.sum(tot_in[...], axis=0)
    at = lax.broadcasted_iota(jnp.int32, (rows, LANES), 0) + lax.rem(me, devs) * rows
    tot = jnp.where(lax.broadcasted_iota(jnp.int32, (rows, LANES), 1) == at, tot, 0.0)
    o_ref[...] = (num / jnp.sum(tot, axis=1, keepdims=True)).astype(jnp.bfloat16)
    all_num.wait_send()
    all_tot.wait_send()


def body(queries, key_pages, value_pages, page_owner, page_local, seq_lengths):
    n = lax.axis_size("seq")
    per, all_heads, head_dim = queries.shape
    pool, kv, page, _ = key_pages.shape
    heads = all_heads // lax.axis_size("tp")
    rows = per * heads
    seqs, slots = page_owner.shape
    devs = PHASE_ROWS // rows
    assert kv == 1 and pool == LANES and head_dim == LANES and seqs == n * per
    tokens = pool * page
    dma = pltpu.SemaphoreType.DMA
    out = pl.pallas_call(
        functools.partial(kernel, n),
        out_shape=pltpu.VMEM((rows, head_dim), jnp.bfloat16),
        in_specs=[pl.BlockSpec(memory_space=pl.ANY)] * 6,
        out_specs=pl.BlockSpec(memory_space=pltpu.VMEM),
        scratch_shapes=[
            pltpu.VMEM(queries.shape, jnp.bfloat16),
            pltpu.VMEM((tokens, head_dim), jnp.bfloat16),
            pltpu.VMEM((tokens, head_dim), jnp.bfloat16),
            pltpu.VMEM((seqs, slots), jnp.int32),
            pltpu.VMEM((seqs, slots), jnp.int32),
            pltpu.SMEM((seqs,), jnp.int32),
            pltpu.VMEM((n, rows, head_dim), jnp.bfloat16),
            pltpu.VMEM((HI, tokens // HI), jnp.float32),
            pltpu.VMEM((n, rows, head_dim), jnp.bfloat16),
            pltpu.VMEM((n // devs, 1, LANES), jnp.float32),
            pltpu.VMEM((n, rows, head_dim), jnp.bfloat16),
            pltpu.VMEM((n, 1, LANES), jnp.float32),
            dma((6,)),
            dma,
            dma,
            dma,
            dma,
            dma,
            dma((WRAP_PHASES,)),
            dma((n,)),
            dma,
            dma,
            dma,
            dma,
            pltpu.SemaphoreType.REGULAR,
            pltpu.SemaphoreType.REGULAR,
            pltpu.SemaphoreType.REGULAR,
            pltpu.SemaphoreType.REGULAR((WRAP,)),
        ],
        compiler_params=pltpu.CompilerParams(collective_id=0, has_side_effects=True),
        name="paged_attention",
    )(
        queries,
        key_pages.reshape(tokens, head_dim),
        value_pages.reshape(tokens, head_dim),
        page_owner,
        page_local,
        seq_lengths,
    )
    return out.reshape(per, heads, head_dim)


def solution(mesh):
    placed = (
        P(("rep", "seq"), None, None),
        P(("rep", "seq"), "tp", None, None),
        P(("rep", "seq"), "tp", None, None),
        P("rep", None),
        P("rep", None),
        P("rep"),
    )
    return jax.shard_map(
        body, mesh=mesh, in_specs=placed, out_specs=P(("rep", "seq"), "tp", None), check_vma=False
    )
```

```python
import functools
import math

import jax
import jax.numpy as jnp
from jax import lax
from jax.experimental import pallas as pl
from jax.experimental.pallas import tpu as pltpu
from jax.sharding import PartitionSpec as P

SHIFT = 8.0
PHASE_ROWS = 128
LANES = 128
HI = 8
WRAP = 6
HOP = 4
WRAP_PHASES = 2
MESH = pl.DeviceIdType.MESH


def kernel(
    n,
    q_hbm,
    k_hbm,
    v_hbm,
    own_hbm,
    loc_hbm,
    len_hbm,
    o_ref,
    q_buf,
    k_buf,
    v_buf,
    own_buf,
    loc_buf,
    len_ref,
    q_all,
    tok_seq,
    num_out,
    tot_out,
    num_in,
    tot_in,
    load_sem,
    low_send,
    up_send,
    up2_send,
    hop_send,
    wrap_send,
    wrap_recv,
    q_recv,
    num_send,
    tot_send,
    num_recv,
    tot_recv,
    up_here,
    up2_here,
    hop_here,
    wrap_here,
):
    z = lax.axis_index("seq")
    tp = lax.axis_index("tp")
    shift = jnp.where(lax.axis_index("rep") + tp == 0, 1, 0)
    me = lax.rem(z + n - shift, n)

    def at_place(p):
        return {"seq": lax.rem(p + shift, n)}

    per, _, head_dim = q_buf.shape
    heads = q_all.shape[1] // per
    rows = per * heads
    seqs, slots = own_buf.shape
    tokens = k_buf.shape[0]
    chunk = tokens // HI
    page = k_buf.shape[0] // (HI * (LANES // HI))
    lows = LANES // HI
    devs = PHASE_ROWS // rows
    phases = n // devs

    loads = [
        pltpu.make_async_copy(src, dst, load_sem.at[i])
        for i, (src, dst) in enumerate(
            [
                (q_hbm, q_buf),
                (own_hbm, own_buf),
                (loc_hbm, loc_buf),
                (k_hbm, k_buf),
                (v_hbm, v_buf),
                (len_hbm, len_ref),
            ]
        )
    ]
    for load in loads:
        load.start()

    barrier = pltpu.get_barrier_semaphore()

    def greet(d, carry):
        pl.semaphore_signal(barrier, inc=1, device_id=at_place(d), device_id_type=MESH)
        return carry

    lax.fori_loop(me + 1, n, greet, 0)

    @pl.when(me >= 1)
    def _():
        pl.semaphore_wait(barrier, me)
        pl.semaphore_signal(up_here, inc=1, device_id=at_place(me - 1), device_id_type=MESH)

    @pl.when(me >= 2)
    def _():
        pl.semaphore_signal(up2_here, inc=1, device_id=at_place(me - 2), device_id_type=MESH)

    half = n // 2
    first_hop = min(half + HOP, n - WRAP)

    @pl.when((me >= first_hop) & (me < n - WRAP))
    def _():
        pl.semaphore_signal(hop_here, inc=1, device_id=at_place(me - HOP), device_id_type=MESH)

    @pl.when(me >= n - WRAP)
    def _():
        pl.semaphore_signal(
            wrap_here.at[me - (n - WRAP)], inc=1, device_id=at_place(0), device_id_type=MESH
        )

    loads[0].wait()
    mine = jnp.zeros((per, heads, head_dim), jnp.float32)
    wide = q_buf[...].astype(jnp.float32)
    for t in range(q_buf.shape[1] // heads):
        mine = jnp.where(tp == t, wide[:, t * heads : (t + 1) * heads, :], mine)
    q_all[me] = mine.reshape(rows, head_dim).astype(jnp.bfloat16)

    def q_copy(j, d, sem):
        return pltpu.make_async_remote_copy(
            src_ref=q_all.at[j],
            dst_ref=q_all.at[j],
            send_sem=sem,
            recv_sem=q_recv.at[j],
            device_id=at_place(d),
            device_id_type=MESH,
        )

    def far(j, p):
        return j - p > half

    @pl.when(far(me, 0))
    def _():
        q_copy(me, 0, low_send).start()

    def send_low(d, carry):
        q_copy(me, d, low_send).start()
        return carry

    lax.fori_loop(jnp.maximum(me - half, 0), me, send_low, 0)

    loads[1].wait()
    loads[2].wait()
    loads[5].wait()
    slot = lax.broadcasted_iota(jnp.int32, (8, slots), 1)
    sub = lax.broadcasted_iota(jnp.int32, (8, slots), 0)

    def tally(g, table):
        own = own_buf[pl.ds(pl.multiple_of(g * 8, 8), 8), :]
        loc = loc_buf[pl.ds(pl.multiple_of(g * 8, 8), 8), :]
        length = jnp.zeros((8, slots), jnp.int32)
        for i in range(8):
            length = jnp.where(sub == i, len_ref[g * 8 + i], length)
        fill = jnp.clip(length - slot * page, 0, page)
        key = jnp.where((own == z) & (fill > 0), loc, -1)
        high = key >> (lows.bit_length() - 1)
        low = key & (lows - 1)
        fill_f = fill.astype(jnp.float32)
        seq_f = (g * 8 + sub).astype(jnp.float32)
        left = [jnp.where(high == h, v, 0.0) for v in (seq_f, fill_f) for h in range(HI)]
        right = [jnp.where(low == l, 1.0, 0.0) for l in range(lows)]
        left = jnp.concatenate(left, axis=0).astype(jnp.bfloat16)
        right = jnp.concatenate(right, axis=0).astype(jnp.bfloat16)
        return table + lax.dot_general(
            left, right, (((1,), (1,)), ((), ())), preferred_element_type=jnp.float32
        )

    table = lax.fori_loop(0, seqs // 8, tally, jnp.zeros((2 * HI * 8, lows * 8), jnp.float32))
    row_id = lax.broadcasted_iota(jnp.int32, table.shape, 0)
    col_id = lax.broadcasted_iota(jnp.int32, table.shape, 1)
    table = jnp.where((row_id & 7) == (col_id & 7), table, 0.0).astype(jnp.bfloat16)
    pick = (
        lax.broadcasted_iota(jnp.int32, (2 * HI, 2 * HI * 8), 1) >> 3
        == lax.broadcasted_iota(jnp.int32, (2 * HI, 2 * HI * 8), 0)
    )
    spread = (
        lax.broadcasted_iota(jnp.int32, (lows * 8, chunk), 0) >> 3
        == lax.broadcasted_iota(jnp.int32, (lows * 8, chunk), 1) // page
    )
    pick = jnp.where(pick, 1.0, 0.0).astype(jnp.bfloat16)
    spread = jnp.where(spread, 1.0, 0.0).astype(jnp.bfloat16)
    small = jnp.dot(pick, table, preferred_element_type=jnp.float32).astype(jnp.bfloat16)
    per_token = jnp.dot(small, spread, preferred_element_type=jnp.float32)
    place = (lax.broadcasted_iota(jnp.int32, (HI, chunk), 1) % page).astype(jnp.float32)
    tok_seq[...] = jnp.where(place < per_token[HI:], per_token[:HI], -1.0)

    @pl.when(me + 1 < n)
    def _():
        pl.semaphore_wait(up_here, 1)
        q_copy(me, me + 1, up_send).start()

    @pl.when(me + 2 < n)
    def _():
        pl.semaphore_wait(up2_here, 1)
        q_copy(me, me + 2, up2_send).start()

    def wrap_copy(g, p):
        return pltpu.make_async_remote_copy(
            src_ref=q_all.at[pl.ds(g * devs, devs)],
            dst_ref=q_all.at[pl.ds(g * devs, devs)],
            send_sem=wrap_send,
            recv_sem=wrap_recv.at[g],
            device_id=at_place(p),
            device_id_type=MESH,
        )

    def hop_copy(p):
        return pltpu.make_async_remote_copy(
            src_ref=q_all.at[pl.ds(0, devs)],
            dst_ref=q_all.at[pl.ds(0, devs)],
            send_sem=hop_send,
            recv_sem=wrap_recv.at[0],
            device_id=at_place(p),
            device_id_type=MESH,
        )

    def goes_up(j):
        limit = jnp.where(j < devs, first_hop, jnp.where(j < WRAP_PHASES * devs, n - WRAP, n))
        return ((j < me) & (me + 2 < limit)) | far(j, me + 2)

    hops = (me + HOP >= first_hop) & (me + HOP < n - WRAP)

    loads[3].wait()
    loads[4].wait()

    def num_copy(d, s):
        return pltpu.make_async_remote_copy(
            src_ref=num_out.at[d],
            dst_ref=num_in.at[s],
            send_sem=num_send,
            recv_sem=num_recv,
            device_id=at_place(d),
            device_id_type=MESH,
        )

    def tot_copy(d, s):
        return pltpu.make_async_remote_copy(
            src_ref=tot_out.at[d // devs],
            dst_ref=tot_in.at[s],
            send_sem=tot_send,
            recv_sem=tot_recv,
            device_id=at_place(d),
            device_id_type=MESH,
        )

    def all_copies(src, dst, send, recv):
        return pltpu.make_async_remote_copy(
            src_ref=src.at[pl.ds(0, n - 1)],
            dst_ref=dst.at[pl.ds(0, n - 1)],
            send_sem=send,
            recv_sem=recv,
            device_id=at_place(me),
            device_id_type=MESH,
        )

    all_num = all_copies(num_in, num_in, num_send, num_recv)
    all_tot = all_copies(tot_in, tot_in, tot_send, tot_recv)

    log2e = math.log2(math.e)
    gain, lift = log2e / math.sqrt(head_dim), SHIFT * log2e
    eye = lax.broadcasted_iota(jnp.int32, (PHASE_ROWS, LANES), 0) == lax.broadcasted_iota(
        jnp.int32, (PHASE_ROWS, LANES), 1
    )

    def give(d, carry):
        @pl.when(d != me)
        def _():
            num_copy(d, me).start()
            tot_copy(d, me).start()

        @pl.when(d == me)
        def _():
            num_in[me] = num_out[me]
            tot_in[me] = tot_out[d // devs]

        return carry

    def phase(g, carry):
        fed = ((g == 0) & (me >= first_hop)) | ((g < WRAP_PHASES) & (me >= n - WRAP))

        @pl.when(fed)
        def _():
            wrap_copy(g, me).wait_recv()

        def arrived(j, carry):
            @pl.when((j != me) & jnp.logical_not(fed))
            def _():
                q_copy(j, me, up_send).wait_recv()

            @pl.when((me == 0) & far(j, 1))
            def _():
                q_copy(j, 1, low_send).start()

            @pl.when(goes_up(j))
            def _():
                q_copy(j, me + 2, up2_send).start()

            return carry

        start = g * devs
        stop = jnp.where(g < phases // 2, start + devs, jnp.where(g == phases // 2, n, start))
        lax.fori_loop(start, stop, arrived, 0)
        @pl.when((g == 0) & hops)
        def _():
            pl.semaphore_wait(hop_here, 1)
            hop_copy(me + HOP).start()

        @pl.when((g == WRAP_PHASES - 1) & (me == 0))
        def _():
            for i in range(WRAP):
                pl.semaphore_wait(wrap_here.at[i], 1)
                wrap_copy(0, n - WRAP + i).start()
            for w in range(1, WRAP_PHASES):
                for i in range(WRAP):
                    wrap_copy(w, n - WRAP + i).start()

        q = q_all[pl.ds(g * devs, devs)].reshape(PHASE_ROWS, head_dim)
        row = lax.broadcasted_iota(jnp.int32, (PHASE_ROWS, 1), 0)
        source = g * devs + row // rows + shift
        source = jnp.where(source >= n, source - n, source)
        row_seq = (source * per + row % rows // heads).astype(jnp.float32)

        def tile(c, sums):
            num, tot = sums
            at = pl.ds(pl.multiple_of(c * chunk, chunk), chunk)
            s = lax.dot_general(
                q, k_buf[at, :], (((1,), (1,)), ((), ())), preferred_element_type=jnp.float32
            )
            w = jnp.exp2(s * gain - lift)
            w = jnp.where(tok_seq[pl.ds(c, 1), :] == row_seq, w, 0.0)
            for i in range(chunk // LANES):
                tot = tot + w[:, i * LANES : (i + 1) * LANES]
            num = num + jnp.dot(
                w.astype(jnp.bfloat16), v_buf[at, :], preferred_element_type=jnp.float32
            )
            return num, tot

        zero = jnp.zeros((PHASE_ROWS, LANES), jnp.float32)
        num, tot = lax.fori_loop(0, HI, tile, (zero, zero), unroll=HI)
        num_out[pl.ds(g * devs, devs)] = num.astype(jnp.bfloat16).reshape(devs, rows, head_dim)
        tot = jnp.sum(tot, axis=1, keepdims=True)
        tot_out[g] = jnp.sum(jnp.where(eye, tot, 0.0), axis=0, keepdims=True)

        late = me >= n - WRAP
        start = jnp.where(late & (g == 1), devs // 2, g * devs)
        stop = jnp.where(late & (g == 0), devs // 2, (g + 1) * devs)
        lax.fori_loop(start, stop, give, 0)
        return carry

    lax.fori_loop(0, phases, phase, 0)

    def sent(sem, count, most):
        for k in range(1, most + 1):

            @pl.when(count == k)
            def _():
                pltpu.make_async_remote_copy(
                    src_ref=q_all.at[pl.ds(0, k)],
                    dst_ref=q_all.at[pl.ds(0, k)],
                    send_sem=sem,
                    recv_sem=q_recv.at[0],
                    device_id=at_place(me),
                    device_id_type=MESH,
                ).wait_send()

    low = jnp.minimum(me, half) + jnp.where(far(me, 0), 1, 0)
    sent(low_send, jnp.where(me == 0, n - half - 2, low), half + 1)
    below = jnp.where(me + 2 < n - WRAP, me - devs, jnp.maximum(me - WRAP_PHASES * devs, 0))
    below = jnp.where(me + 2 < first_hop, me, below)
    up2 = jnp.where(me + 2 < n, below + 1, 0) + jnp.maximum(n - 3 - me - half, 0)
    sent(up2_send, up2, n)

    @pl.when(me + 1 < n)
    def _():
        q_copy(me, me, up_send).wait_send()

    @pl.when(hops)
    def _():
        hop_copy(me).wait_send()

    @pl.when(me == 0)
    def _():
        fed_rows = WRAP_PHASES * WRAP * devs * rows
        pltpu.make_async_remote_copy(
            src_ref=k_buf.at[pl.ds(0, fed_rows)],
            dst_ref=k_buf.at[pl.ds(0, fed_rows)],
            send_sem=wrap_send,
            recv_sem=q_recv.at[0],
            device_id=at_place(me),
            device_id_type=MESH,
        ).wait_send()

    all_num.wait_recv()
    all_tot.wait_recv()
    num = jnp.sum(num_in[...].astype(jnp.float32), axis=0)
    tot = jnp.sum(tot_in[...], axis=0)
    at = lax.broadcasted_iota(jnp.int32, (rows, LANES), 0) + lax.rem(me, devs) * rows
    tot = jnp.where(lax.broadcasted_iota(jnp.int32, (rows, LANES), 1) == at, tot, 0.0)
    o_ref[...] = (num / jnp.sum(tot, axis=1, keepdims=True)).astype(jnp.bfloat16)
    all_num.wait_send()
    all_tot.wait_send()


def body(queries, key_pages, value_pages, page_owner, page_local, seq_lengths):
    n = lax.axis_size("seq")
    per, all_heads, head_dim = queries.shape
    pool, kv, page, _ = key_pages.shape
    heads = all_heads // lax.axis_size("tp")
    rows = per * heads
    seqs, slots = page_owner.shape
    devs = PHASE_ROWS // rows
    assert kv == 1 and pool == LANES and head_dim == LANES and seqs == n * per
    tokens = pool * page
    dma = pltpu.SemaphoreType.DMA
    out = pl.pallas_call(
        functools.partial(kernel, n),
        out_shape=pltpu.VMEM((rows, head_dim), jnp.bfloat16),
        in_specs=[pl.BlockSpec(memory_space=pl.ANY)] * 6,
        out_specs=pl.BlockSpec(memory_space=pltpu.VMEM),
        scratch_shapes=[
            pltpu.VMEM(queries.shape, jnp.bfloat16),
            pltpu.VMEM((tokens, head_dim), jnp.bfloat16),
            pltpu.VMEM((tokens, head_dim), jnp.bfloat16),
            pltpu.VMEM((seqs, slots), jnp.int32),
            pltpu.VMEM((seqs, slots), jnp.int32),
            pltpu.SMEM((seqs,), jnp.int32),
            pltpu.VMEM((n, rows, head_dim), jnp.bfloat16),
            pltpu.VMEM((HI, tokens // HI), jnp.float32),
            pltpu.VMEM((n, rows, head_dim), jnp.bfloat16),
            pltpu.VMEM((n // devs, 1, LANES), jnp.float32),
            pltpu.VMEM((n, rows, head_dim), jnp.bfloat16),
            pltpu.VMEM((n, 1, LANES), jnp.float32),
            dma((6,)),
            dma,
            dma,
            dma,
            dma,
            dma,
            dma((WRAP_PHASES,)),
            dma((n,)),
            dma,
            dma,
            dma,
            dma,
            pltpu.SemaphoreType.REGULAR,
            pltpu.SemaphoreType.REGULAR,
            pltpu.SemaphoreType.REGULAR,
            pltpu.SemaphoreType.REGULAR((WRAP,)),
        ],
        compiler_params=pltpu.CompilerParams(collective_id=0, has_side_effects=True),
        name="paged_attention",
    )(
        queries,
        key_pages.reshape(tokens, head_dim),
        value_pages.reshape(tokens, head_dim),
        page_owner,
        page_local,
        seq_lengths,
    )
    return out.reshape(per, heads, head_dim)


def solution(mesh):
    placed = (
        P(("rep", "seq"), None, None),
        P(("rep", "seq"), "tp", None, None),
        P(("rep", "seq"), "tp", None, None),
        P("rep", None),
        P("rep", None),
        P("rep"),
    )
    return jax.shard_map(
        body, mesh=mesh, in_specs=placed, out_specs=P(("rep", "seq"), "tp", None), check_vma=False
    )
```

```python
import functools
import math

import jax
import jax.numpy as jnp
from jax import lax
from jax.experimental import pallas as pl
from jax.experimental.pallas import tpu as pltpu
from jax.sharding import PartitionSpec as P

SHIFT = 8.0
PHASE_ROWS = 128
LANES = 128
HI = 8
WRAP = 6
HOP = 4
WRAP_PHASES = 2
MESH = pl.DeviceIdType.MESH


def kernel(
    n,
    q_hbm,
    k_hbm,
    v_hbm,
    own_hbm,
    loc_hbm,
    len_hbm,
    o_ref,
    q_buf,
    k_buf,
    v_buf,
    own_buf,
    loc_buf,
    len_ref,
    q_all,
    tok_seq,
    num_out,
    tot_out,
    num_in,
    tot_in,
    load_sem,
    low_send,
    up_send,
    up2_send,
    hop_send,
    wrap_send,
    wrap_recv,
    q_recv,
    num_send,
    tot_send,
    num_recv,
    tot_recv,
    up_here,
    up2_here,
    hop_here,
    wrap_here,
):
    z = lax.axis_index("seq")
    tp = lax.axis_index("tp")
    shift = jnp.where(lax.axis_index("rep") + tp == 0, 1, 0)
    me = lax.rem(z + n - shift, n)

    def at_place(p):
        return {"seq": lax.rem(p + shift, n)}

    per, _, head_dim = q_buf.shape
    heads = q_all.shape[1] // per
    rows = per * heads
    seqs, slots = own_buf.shape
    tokens = k_buf.shape[0]
    chunk = tokens // HI
    page = k_buf.shape[0] // (HI * (LANES // HI))
    lows = LANES // HI
    devs = PHASE_ROWS // rows
    phases = n // devs

    loads = [
        pltpu.make_async_copy(src, dst, load_sem.at[i])
        for i, (src, dst) in enumerate(
            [
                (q_hbm, q_buf),
                (own_hbm, own_buf),
                (loc_hbm, loc_buf),
                (k_hbm, k_buf),
                (v_hbm, v_buf),
                (len_hbm, len_ref),
            ]
        )
    ]
    for load in loads:
        load.start()

    barrier = pltpu.get_barrier_semaphore()

    def greet(d, carry):
        pl.semaphore_signal(barrier, inc=1, device_id=at_place(d), device_id_type=MESH)
        return carry

    lax.fori_loop(me + 1, n, greet, 0)

    @pl.when(me >= 1)
    def _():
        pl.semaphore_wait(barrier, me)
        pl.semaphore_signal(up_here, inc=1, device_id=at_place(me - 1), device_id_type=MESH)

    @pl.when(me >= 2)
    def _():
        pl.semaphore_signal(up2_here, inc=1, device_id=at_place(me - 2), device_id_type=MESH)

    half = n // 2
    first_hop = min(half + HOP, n - WRAP)

    @pl.when((me >= first_hop) & (me < n - WRAP))
    def _():
        pl.semaphore_signal(hop_here, inc=1, device_id=at_place(me - HOP), device_id_type=MESH)

    @pl.when(me >= n - WRAP)
    def _():
        pl.semaphore_signal(
            wrap_here.at[me - (n - WRAP)], inc=1, device_id=at_place(0), device_id_type=MESH
        )

    loads[0].wait()
    mine = jnp.zeros((per, heads, head_dim), jnp.float32)
    wide = q_buf[...].astype(jnp.float32)
    for t in range(q_buf.shape[1] // heads):
        mine = jnp.where(tp == t, wide[:, t * heads : (t + 1) * heads, :], mine)
    q_all[me] = mine.reshape(rows, head_dim).astype(jnp.bfloat16)

    def q_copy(j, d, sem):
        return pltpu.make_async_remote_copy(
            src_ref=q_all.at[j],
            dst_ref=q_all.at[j],
            send_sem=sem,
            recv_sem=q_recv.at[j],
            device_id=at_place(d),
            device_id_type=MESH,
        )

    def far(j, p):
        return j - p > half

    @pl.when(far(me, 0))
    def _():
        q_copy(me, 0, low_send).start()

    def send_low(d, carry):
        q_copy(me, d, low_send).start()
        return carry

    lax.fori_loop(jnp.maximum(me - half, 0), me, send_low, 0)

    loads[1].wait()
    loads[2].wait()
    loads[5].wait()
    slot = lax.broadcasted_iota(jnp.int32, (8, slots), 1)
    sub = lax.broadcasted_iota(jnp.int32, (8, slots), 0)

    def tally(g, table):
        own = own_buf[pl.ds(pl.multiple_of(g * 8, 8), 8), :]
        loc = loc_buf[pl.ds(pl.multiple_of(g * 8, 8), 8), :]
        length = jnp.zeros((8, slots), jnp.int32)
        for i in range(8):
            length = jnp.where(sub == i, len_ref[g * 8 + i], length)
        fill = jnp.clip(length - slot * page, 0, page)
        key = jnp.where((own == z) & (fill > 0), loc, -1)
        high = key >> (lows.bit_length() - 1)
        low = key & (lows - 1)
        fill_f = fill.astype(jnp.float32)
        seq_f = (g * 8 + sub).astype(jnp.float32)
        left = [jnp.where(high == h, v, 0.0) for v in (seq_f, fill_f) for h in range(HI)]
        right = [jnp.where(low == l, 1.0, 0.0) for l in range(lows)]
        left = jnp.concatenate(left, axis=0).astype(jnp.bfloat16)
        right = jnp.concatenate(right, axis=0).astype(jnp.bfloat16)
        return table + lax.dot_general(
            left, right, (((1,), (1,)), ((), ())), preferred_element_type=jnp.float32
        )

    table = lax.fori_loop(0, seqs // 8, tally, jnp.zeros((2 * HI * 8, lows * 8), jnp.float32))
    row_id = lax.broadcasted_iota(jnp.int32, table.shape, 0)
    col_id = lax.broadcasted_iota(jnp.int32, table.shape, 1)
    table = jnp.where((row_id & 7) == (col_id & 7), table, 0.0).astype(jnp.bfloat16)
    pick = (
        lax.broadcasted_iota(jnp.int32, (2 * HI, 2 * HI * 8), 1) >> 3
        == lax.broadcasted_iota(jnp.int32, (2 * HI, 2 * HI * 8), 0)
    )
    spread = (
        lax.broadcasted_iota(jnp.int32, (lows * 8, chunk), 0) >> 3
        == lax.broadcasted_iota(jnp.int32, (lows * 8, chunk), 1) // page
    )
    pick = jnp.where(pick, 1.0, 0.0).astype(jnp.bfloat16)
    spread = jnp.where(spread, 1.0, 0.0).astype(jnp.bfloat16)
    small = jnp.dot(pick, table, preferred_element_type=jnp.float32).astype(jnp.bfloat16)
    per_token = jnp.dot(small, spread, preferred_element_type=jnp.float32)
    place = (lax.broadcasted_iota(jnp.int32, (HI, chunk), 1) % page).astype(jnp.float32)
    tok_seq[...] = jnp.where(place < per_token[HI:], per_token[:HI], -1.0)

    @pl.when(me + 1 < n)
    def _():
        pl.semaphore_wait(up_here, 1)
        q_copy(me, me + 1, up_send).start()

    @pl.when(me + 2 < n)
    def _():
        pl.semaphore_wait(up2_here, 1)
        q_copy(me, me + 2, up2_send).start()

    def wrap_copy(g, p):
        return pltpu.make_async_remote_copy(
            src_ref=q_all.at[pl.ds(g * devs, devs)],
            dst_ref=q_all.at[pl.ds(g * devs, devs)],
            send_sem=wrap_send,
            recv_sem=wrap_recv.at[g],
            device_id=at_place(p),
            device_id_type=MESH,
        )

    def hop_copy(p):
        return pltpu.make_async_remote_copy(
            src_ref=q_all.at[pl.ds(0, devs)],
            dst_ref=q_all.at[pl.ds(0, devs)],
            send_sem=hop_send,
            recv_sem=wrap_recv.at[0],
            device_id=at_place(p),
            device_id_type=MESH,
        )

    def goes_up(j):
        limit = jnp.where(j < devs, first_hop, jnp.where(j < WRAP_PHASES * devs, n - WRAP, n))
        return ((j < me) & (me + 2 < limit)) | far(j, me + 2)

    hops = (me + HOP >= first_hop) & (me + HOP < n - WRAP)

    loads[3].wait()
    loads[4].wait()

    def num_copy(d, s):
        return pltpu.make_async_remote_copy(
            src_ref=num_out.at[d],
            dst_ref=num_in.at[s],
            send_sem=num_send,
            recv_sem=num_recv,
            device_id=at_place(d),
            device_id_type=MESH,
        )

    def tot_copy(d, s):
        return pltpu.make_async_remote_copy(
            src_ref=tot_out.at[d // devs],
            dst_ref=tot_in.at[s],
            send_sem=tot_send,
            recv_sem=tot_recv,
            device_id=at_place(d),
            device_id_type=MESH,
        )

    def all_copies(src, dst, send, recv):
        return pltpu.make_async_remote_copy(
            src_ref=src.at[pl.ds(0, n - 1)],
            dst_ref=dst.at[pl.ds(0, n - 1)],
            send_sem=send,
            recv_sem=recv,
            device_id=at_place(me),
            device_id_type=MESH,
        )

    all_num = all_copies(num_in, num_in, num_send, num_recv)
    all_tot = all_copies(tot_in, tot_in, tot_send, tot_recv)

    log2e = math.log2(math.e)
    gain, lift = log2e / math.sqrt(head_dim), SHIFT * log2e
    eye = lax.broadcasted_iota(jnp.int32, (PHASE_ROWS, LANES), 0) == lax.broadcasted_iota(
        jnp.int32, (PHASE_ROWS, LANES), 1
    )

    def give(d, carry):
        @pl.when(d != me)
        def _():
            num_copy(d, me).start()
            tot_copy(d, me).start()

        @pl.when(d == me)
        def _():
            num_in[me] = num_out[me]
            tot_in[me] = tot_out[d // devs]

        return carry

    def phase(g, carry):
        fed = ((g == 0) & (me >= first_hop)) | ((g < WRAP_PHASES) & (me >= n - WRAP))

        @pl.when(fed)
        def _():
            wrap_copy(g, me).wait_recv()

        def arrived(j, carry):
            @pl.when((j != me) & jnp.logical_not(fed))
            def _():
                q_copy(j, me, up_send).wait_recv()

            @pl.when((me == 0) & far(j, 1))
            def _():
                q_copy(j, 1, low_send).start()

            @pl.when(goes_up(j))
            def _():
                q_copy(j, me + 2, up2_send).start()

            return carry

        start = g * devs
        stop = jnp.where(g < phases // 2, start + devs, jnp.where(g == phases // 2, n, start))
        lax.fori_loop(start, stop, arrived, 0)
        @pl.when((g == 0) & hops)
        def _():
            pl.semaphore_wait(hop_here, 1)
            hop_copy(me + HOP).start()

        @pl.when((g == WRAP_PHASES - 1) & (me == 0))
        def _():
            for i in range(WRAP):
                pl.semaphore_wait(wrap_here.at[i], 1)
                wrap_copy(0, n - WRAP + i).start()
            for w in range(1, WRAP_PHASES):
                for i in range(WRAP):
                    wrap_copy(w, n - WRAP + i).start()

        q = q_all[pl.ds(g * devs, devs)].reshape(PHASE_ROWS, head_dim)
        row = lax.broadcasted_iota(jnp.int32, (PHASE_ROWS, 1), 0)
        source = g * devs + row // rows + shift
        source = jnp.where(source >= n, source - n, source)
        row_seq = (source * per + row % rows // heads).astype(jnp.float32)

        def tile(c, sums):
            num, tot = sums
            at = pl.ds(pl.multiple_of(c * chunk, chunk), chunk)
            s = lax.dot_general(
                q, k_buf[at, :], (((1,), (1,)), ((), ())), preferred_element_type=jnp.float32
            )
            w = jnp.exp2(s * gain - lift)
            w = jnp.where(tok_seq[pl.ds(c, 1), :] == row_seq, w, 0.0)
            for i in range(chunk // LANES):
                tot = tot + w[:, i * LANES : (i + 1) * LANES]
            num = num + jnp.dot(
                w.astype(jnp.bfloat16), v_buf[at, :], preferred_element_type=jnp.float32
            )
            return num, tot

        zero = jnp.zeros((PHASE_ROWS, LANES), jnp.float32)
        num, tot = lax.fori_loop(0, HI, tile, (zero, zero), unroll=HI)
        num_out[pl.ds(g * devs, devs)] = num.astype(jnp.bfloat16).reshape(devs, rows, head_dim)
        tot = jnp.sum(tot, axis=1, keepdims=True)
        tot_out[g] = jnp.sum(jnp.where(eye, tot, 0.0), axis=0, keepdims=True)

        at_once = devs * 5 // 8
        start = jnp.where(g == 1, at_once, g * devs)
        stop = jnp.where(g == 0, at_once, (g + 1) * devs)
        lax.fori_loop(start, stop, give, 0)
        return carry

    lax.fori_loop(0, phases, phase, 0)

    def sent(sem, count, most):
        for k in range(1, most + 1):

            @pl.when(count == k)
            def _():
                pltpu.make_async_remote_copy(
                    src_ref=q_all.at[pl.ds(0, k)],
                    dst_ref=q_all.at[pl.ds(0, k)],
                    send_sem=sem,
                    recv_sem=q_recv.at[0],
                    device_id=at_place(me),
                    device_id_type=MESH,
                ).wait_send()

    low = jnp.minimum(me, half) + jnp.where(far(me, 0), 1, 0)
    sent(low_send, jnp.where(me == 0, n - half - 2, low), half + 1)
    below = jnp.where(me + 2 < n - WRAP, me - devs, jnp.maximum(me - WRAP_PHASES * devs, 0))
    below = jnp.where(me + 2 < first_hop, me, below)
    up2 = jnp.where(me + 2 < n, below + 1, 0) + jnp.maximum(n - 3 - me - half, 0)
    sent(up2_send, up2, n)

    @pl.when(me + 1 < n)
    def _():
        q_copy(me, me, up_send).wait_send()

    @pl.when(hops)
    def _():
        hop_copy(me).wait_send()

    @pl.when(me == 0)
    def _():
        fed_rows = WRAP_PHASES * WRAP * devs * rows
        pltpu.make_async_remote_copy(
            src_ref=k_buf.at[pl.ds(0, fed_rows)],
            dst_ref=k_buf.at[pl.ds(0, fed_rows)],
            send_sem=wrap_send,
            recv_sem=q_recv.at[0],
            device_id=at_place(me),
            device_id_type=MESH,
        ).wait_send()

    all_num.wait_recv()
    all_tot.wait_recv()
    num = jnp.sum(num_in[...].astype(jnp.float32), axis=0)
    tot = jnp.sum(tot_in[...], axis=0)
    at = lax.broadcasted_iota(jnp.int32, (rows, LANES), 0) + lax.rem(me, devs) * rows
    tot = jnp.where(lax.broadcasted_iota(jnp.int32, (rows, LANES), 1) == at, tot, 0.0)
    o_ref[...] = (num / jnp.sum(tot, axis=1, keepdims=True)).astype(jnp.bfloat16)
    all_num.wait_send()
    all_tot.wait_send()


def body(queries, key_pages, value_pages, page_owner, page_local, seq_lengths):
    n = lax.axis_size("seq")
    per, all_heads, head_dim = queries.shape
    pool, kv, page, _ = key_pages.shape
    heads = all_heads // lax.axis_size("tp")
    rows = per * heads
    seqs, slots = page_owner.shape
    devs = PHASE_ROWS // rows
    assert kv == 1 and pool == LANES and head_dim == LANES and seqs == n * per
    tokens = pool * page
    dma = pltpu.SemaphoreType.DMA
    out = pl.pallas_call(
        functools.partial(kernel, n),
        out_shape=pltpu.VMEM((rows, head_dim), jnp.bfloat16),
        in_specs=[pl.BlockSpec(memory_space=pl.ANY)] * 6,
        out_specs=pl.BlockSpec(memory_space=pltpu.VMEM),
        scratch_shapes=[
            pltpu.VMEM(queries.shape, jnp.bfloat16),
            pltpu.VMEM((tokens, head_dim), jnp.bfloat16),
            pltpu.VMEM((tokens, head_dim), jnp.bfloat16),
            pltpu.VMEM((seqs, slots), jnp.int32),
            pltpu.VMEM((seqs, slots), jnp.int32),
            pltpu.SMEM((seqs,), jnp.int32),
            pltpu.VMEM((n, rows, head_dim), jnp.bfloat16),
            pltpu.VMEM((HI, tokens // HI), jnp.float32),
            pltpu.VMEM((n, rows, head_dim), jnp.bfloat16),
            pltpu.VMEM((n // devs, 1, LANES), jnp.float32),
            pltpu.VMEM((n, rows, head_dim), jnp.bfloat16),
            pltpu.VMEM((n, 1, LANES), jnp.float32),
            dma((6,)),
            dma,
            dma,
            dma,
            dma,
            dma,
            dma((WRAP_PHASES,)),
            dma((n,)),
            dma,
            dma,
            dma,
            dma,
            pltpu.SemaphoreType.REGULAR,
            pltpu.SemaphoreType.REGULAR,
            pltpu.SemaphoreType.REGULAR,
            pltpu.SemaphoreType.REGULAR((WRAP,)),
        ],
        compiler_params=pltpu.CompilerParams(collective_id=0, has_side_effects=True),
        name="paged_attention",
    )(
        queries,
        key_pages.reshape(tokens, head_dim),
        value_pages.reshape(tokens, head_dim),
        page_owner,
        page_local,
        seq_lengths,
    )
    return out.reshape(per, heads, head_dim)


def solution(mesh):
    placed = (
        P(("rep", "seq"), None, None),
        P(("rep", "seq"), "tp", None, None),
        P(("rep", "seq"), "tp", None, None),
        P("rep", None),
        P("rep", None),
        P("rep"),
    )
    return jax.shard_map(
        body, mesh=mesh, in_specs=placed, out_specs=P(("rep", "seq"), "tp", None), check_vma=False
    )
```

```python
import functools
import math

import jax
import jax.numpy as jnp
from jax import lax
from jax.experimental import pallas as pl
from jax.experimental.pallas import tpu as pltpu
from jax.sharding import PartitionSpec as P

SHIFT = 8.0
PHASE_ROWS = 128
LANES = 128
HI = 8
WRAP = 6
HOP = 4
WRAP_PHASES = 2
MESH = pl.DeviceIdType.MESH


def kernel(
    n,
    q_hbm,
    k_hbm,
    v_hbm,
    own_hbm,
    loc_hbm,
    len_hbm,
    o_ref,
    q_buf,
    k_buf,
    v_buf,
    own_buf,
    loc_buf,
    len_ref,
    q_all,
    tok_seq,
    num_out,
    tot_out,
    num_in,
    tot_in,
    load_sem,
    low_send,
    up_send,
    up2_send,
    hop_send,
    wrap_send,
    wrap_recv,
    q_recv,
    num_send,
    tot_send,
    num_recv,
    tot_recv,
    up_here,
    up2_here,
    hop_here,
    wrap_here,
):
    z = lax.axis_index("seq")
    tp = lax.axis_index("tp")
    shift = jnp.where(lax.axis_index("rep") + tp == 0, 1, 0)
    me = lax.rem(z + n - shift, n)

    def at_place(p):
        return {"seq": lax.rem(p + shift, n)}

    per, _, head_dim = q_buf.shape
    heads = q_all.shape[1] // per
    rows = per * heads
    seqs, slots = own_buf.shape
    tokens = k_buf.shape[0]
    chunk = tokens // HI
    page = k_buf.shape[0] // (HI * (LANES // HI))
    lows = LANES // HI
    devs = PHASE_ROWS // rows
    phases = n // devs

    loads = [
        pltpu.make_async_copy(src, dst, load_sem.at[i])
        for i, (src, dst) in enumerate(
            [
                (q_hbm, q_buf),
                (own_hbm, own_buf),
                (loc_hbm, loc_buf),
                (k_hbm, k_buf),
                (v_hbm, v_buf),
                (len_hbm, len_ref),
            ]
        )
    ]
    for load in loads:
        load.start()

    barrier = pltpu.get_barrier_semaphore()

    def greet(d, carry):
        pl.semaphore_signal(barrier, inc=1, device_id=at_place(d), device_id_type=MESH)
        return carry

    lax.fori_loop(me + 1, n, greet, 0)

    @pl.when(me >= 1)
    def _():
        pl.semaphore_wait(barrier, me)
        pl.semaphore_signal(up_here, inc=1, device_id=at_place(me - 1), device_id_type=MESH)

    @pl.when(me >= 2)
    def _():
        pl.semaphore_signal(up2_here, inc=1, device_id=at_place(me - 2), device_id_type=MESH)

    half = n // 2
    first_hop = min(half + HOP, n - WRAP)

    @pl.when((me >= first_hop) & (me < n - WRAP))
    def _():
        pl.semaphore_signal(hop_here, inc=1, device_id=at_place(me - HOP), device_id_type=MESH)

    @pl.when(me >= n - WRAP)
    def _():
        pl.semaphore_signal(
            wrap_here.at[me - (n - WRAP)], inc=1, device_id=at_place(0), device_id_type=MESH
        )

    loads[0].wait()
    mine = jnp.zeros((per, heads, head_dim), jnp.float32)
    wide = q_buf[...].astype(jnp.float32)
    for t in range(q_buf.shape[1] // heads):
        mine = jnp.where(tp == t, wide[:, t * heads : (t + 1) * heads, :], mine)
    q_all[me] = mine.reshape(rows, head_dim).astype(jnp.bfloat16)

    def q_copy(j, d, sem):
        return pltpu.make_async_remote_copy(
            src_ref=q_all.at[j],
            dst_ref=q_all.at[j],
            send_sem=sem,
            recv_sem=q_recv.at[j],
            device_id=at_place(d),
            device_id_type=MESH,
        )

    def far(j, p):
        return j - p > half

    @pl.when(far(me, 0))
    def _():
        q_copy(me, 0, low_send).start()

    def send_low(d, carry):
        q_copy(me, d, low_send).start()
        return carry

    lax.fori_loop(jnp.maximum(me - half, 0), me, send_low, 0)

    loads[1].wait()
    loads[2].wait()
    loads[5].wait()
    slot = lax.broadcasted_iota(jnp.int32, (8, slots), 1)
    sub = lax.broadcasted_iota(jnp.int32, (8, slots), 0)

    def tally(g, table):
        own = own_buf[pl.ds(pl.multiple_of(g * 8, 8), 8), :]
        loc = loc_buf[pl.ds(pl.multiple_of(g * 8, 8), 8), :]
        length = jnp.zeros((8, slots), jnp.int32)
        for i in range(8):
            length = jnp.where(sub == i, len_ref[g * 8 + i], length)
        fill = jnp.clip(length - slot * page, 0, page)
        key = jnp.where((own == z) & (fill > 0), loc, -1)
        high = key >> (lows.bit_length() - 1)
        low = key & (lows - 1)
        fill_f = fill.astype(jnp.float32)
        seq_f = (g * 8 + sub).astype(jnp.float32)
        left = [jnp.where(high == h, v, 0.0) for v in (seq_f, fill_f) for h in range(HI)]
        right = [jnp.where(low == l, 1.0, 0.0) for l in range(lows)]
        left = jnp.concatenate(left, axis=0).astype(jnp.bfloat16)
        right = jnp.concatenate(right, axis=0).astype(jnp.bfloat16)
        return table + lax.dot_general(
            left, right, (((1,), (1,)), ((), ())), preferred_element_type=jnp.float32
        )

    table = lax.fori_loop(0, seqs // 8, tally, jnp.zeros((2 * HI * 8, lows * 8), jnp.float32))
    row_id = lax.broadcasted_iota(jnp.int32, table.shape, 0)
    col_id = lax.broadcasted_iota(jnp.int32, table.shape, 1)
    table = jnp.where((row_id & 7) == (col_id & 7), table, 0.0).astype(jnp.bfloat16)
    pick = (
        lax.broadcasted_iota(jnp.int32, (2 * HI, 2 * HI * 8), 1) >> 3
        == lax.broadcasted_iota(jnp.int32, (2 * HI, 2 * HI * 8), 0)
    )
    spread = (
        lax.broadcasted_iota(jnp.int32, (lows * 8, chunk), 0) >> 3
        == lax.broadcasted_iota(jnp.int32, (lows * 8, chunk), 1) // page
    )
    pick = jnp.where(pick, 1.0, 0.0).astype(jnp.bfloat16)
    spread = jnp.where(spread, 1.0, 0.0).astype(jnp.bfloat16)
    small = jnp.dot(pick, table, preferred_element_type=jnp.float32).astype(jnp.bfloat16)
    per_token = jnp.dot(small, spread, preferred_element_type=jnp.float32)
    place = (lax.broadcasted_iota(jnp.int32, (HI, chunk), 1) % page).astype(jnp.float32)
    tok_seq[...] = jnp.where(place < per_token[HI:], per_token[:HI], -1.0)

    @pl.when(me + 1 < n)
    def _():
        pl.semaphore_wait(up_here, 1)
        q_copy(me, me + 1, up_send).start()

    @pl.when(me + 2 < n)
    def _():
        pl.semaphore_wait(up2_here, 1)
        q_copy(me, me + 2, up2_send).start()

    def wrap_copy(g, p):
        return pltpu.make_async_remote_copy(
            src_ref=q_all.at[pl.ds(g * devs, devs)],
            dst_ref=q_all.at[pl.ds(g * devs, devs)],
            send_sem=wrap_send,
            recv_sem=wrap_recv.at[g],
            device_id=at_place(p),
            device_id_type=MESH,
        )

    def hop_copy(p):
        return pltpu.make_async_remote_copy(
            src_ref=q_all.at[pl.ds(0, devs)],
            dst_ref=q_all.at[pl.ds(0, devs)],
            send_sem=hop_send,
            recv_sem=wrap_recv.at[0],
            device_id=at_place(p),
            device_id_type=MESH,
        )

    def goes_up(j):
        limit = jnp.where(j < devs, first_hop, jnp.where(j < WRAP_PHASES * devs, n - WRAP, n))
        return ((j < me) & (me + 2 < limit)) | far(j, me + 2)

    hops = (me + HOP >= first_hop) & (me + HOP < n - WRAP)

    loads[3].wait()
    loads[4].wait()

    def num_copy(d, s):
        return pltpu.make_async_remote_copy(
            src_ref=num_out.at[d],
            dst_ref=num_in.at[s],
            send_sem=num_send,
            recv_sem=num_recv,
            device_id=at_place(d),
            device_id_type=MESH,
        )

    def tot_copy(d, s):
        return pltpu.make_async_remote_copy(
            src_ref=tot_out.at[d // devs],
            dst_ref=tot_in.at[s],
            send_sem=tot_send,
            recv_sem=tot_recv,
            device_id=at_place(d),
            device_id_type=MESH,
        )

    def all_copies(src, dst, send, recv):
        return pltpu.make_async_remote_copy(
            src_ref=src.at[pl.ds(0, n - 1)],
            dst_ref=dst.at[pl.ds(0, n - 1)],
            send_sem=send,
            recv_sem=recv,
            device_id=at_place(me),
            device_id_type=MESH,
        )

    all_num = all_copies(num_in, num_in, num_send, num_recv)
    all_tot = all_copies(tot_in, tot_in, tot_send, tot_recv)

    log2e = math.log2(math.e)
    gain, lift = log2e / math.sqrt(head_dim), SHIFT * log2e
    eye = lax.broadcasted_iota(jnp.int32, (PHASE_ROWS, LANES), 0) == lax.broadcasted_iota(
        jnp.int32, (PHASE_ROWS, LANES), 1
    )

    def give(d, carry):
        @pl.when(d != me)
        def _():
            num_copy(d, me).start()
            tot_copy(d, me).start()

        @pl.when(d == me)
        def _():
            num_in[me] = num_out[me]
            tot_in[me] = tot_out[d // devs]

        return carry

    def phase(g, carry):
        fed = ((g == 0) & (me >= first_hop)) | ((g < WRAP_PHASES) & (me >= n - WRAP))

        @pl.when(fed)
        def _():
            wrap_copy(g, me).wait_recv()

        def arrived(j, carry):
            @pl.when((j != me) & jnp.logical_not(fed))
            def _():
                q_copy(j, me, up_send).wait_recv()

            @pl.when((me == 0) & far(j, 1))
            def _():
                q_copy(j, 1, low_send).start()

            @pl.when(goes_up(j))
            def _():
                q_copy(j, me + 2, up2_send).start()

            return carry

        start = g * devs
        stop = jnp.where(g < phases // 2, start + devs, jnp.where(g == phases // 2, n, start))
        lax.fori_loop(start, stop, arrived, 0)
        @pl.when((g == 0) & hops)
        def _():
            pl.semaphore_wait(hop_here, 1)
            hop_copy(me + HOP).start()

        @pl.when((g == WRAP_PHASES - 1) & (me == 0))
        def _():
            for i in range(WRAP):
                pl.semaphore_wait(wrap_here.at[i], 1)
                wrap_copy(0, n - WRAP + i).start()
            for w in range(1, WRAP_PHASES):
                for i in range(WRAP):
                    wrap_copy(w, n - WRAP + i).start()

        q = q_all[pl.ds(g * devs, devs)].reshape(PHASE_ROWS, head_dim)
        row = lax.broadcasted_iota(jnp.int32, (PHASE_ROWS, 1), 0)
        source = g * devs + row // rows + shift
        source = jnp.where(source >= n, source - n, source)
        row_seq = (source * per + row % rows // heads).astype(jnp.float32)

        def tile(c, sums):
            num, tot = sums
            at = pl.ds(pl.multiple_of(c * chunk, chunk), chunk)
            s = lax.dot_general(
                q, k_buf[at, :], (((1,), (1,)), ((), ())), preferred_element_type=jnp.float32
            )
            w = jnp.exp2(s * gain - lift)
            w = jnp.where(tok_seq[pl.ds(c, 1), :] == row_seq, w, 0.0)
            for i in range(chunk // LANES):
                tot = tot + w[:, i * LANES : (i + 1) * LANES]
            num = num + jnp.dot(
                w.astype(jnp.bfloat16), v_buf[at, :], preferred_element_type=jnp.float32
            )
            return num, tot

        zero = jnp.zeros((PHASE_ROWS, LANES), jnp.float32)
        num, tot = lax.fori_loop(0, HI, tile, (zero, zero), unroll=HI)
        num_out[pl.ds(g * devs, devs)] = num.astype(jnp.bfloat16).reshape(devs, rows, head_dim)
        tot = jnp.sum(tot, axis=1, keepdims=True)
        tot_out[g] = jnp.sum(jnp.where(eye, tot, 0.0), axis=0, keepdims=True)

        holds = (me < n - WRAP - 2) | (me >= n - WRAP)
        start = jnp.where(holds & (g == 1), devs // 2, g * devs)
        stop = jnp.where(holds & (g == 0), devs // 2, (g + 1) * devs)
        lax.fori_loop(start, stop, give, 0)
        return carry

    lax.fori_loop(0, phases, phase, 0)

    def sent(sem, count, most):
        for k in range(1, most + 1):

            @pl.when(count == k)
            def _():
                pltpu.make_async_remote_copy(
                    src_ref=q_all.at[pl.ds(0, k)],
                    dst_ref=q_all.at[pl.ds(0, k)],
                    send_sem=sem,
                    recv_sem=q_recv.at[0],
                    device_id=at_place(me),
                    device_id_type=MESH,
                ).wait_send()

    low = jnp.minimum(me, half) + jnp.where(far(me, 0), 1, 0)
    sent(low_send, jnp.where(me == 0, n - half - 2, low), half + 1)
    below = jnp.where(me + 2 < n - WRAP, me - devs, jnp.maximum(me - WRAP_PHASES * devs, 0))
    below = jnp.where(me + 2 < first_hop, me, below)
    up2 = jnp.where(me + 2 < n, below + 1, 0) + jnp.maximum(n - 3 - me - half, 0)
    sent(up2_send, up2, n)

    @pl.when(me + 1 < n)
    def _():
        q_copy(me, me, up_send).wait_send()

    @pl.when(hops)
    def _():
        hop_copy(me).wait_send()

    @pl.when(me == 0)
    def _():
        fed_rows = WRAP_PHASES * WRAP * devs * rows
        pltpu.make_async_remote_copy(
            src_ref=k_buf.at[pl.ds(0, fed_rows)],
            dst_ref=k_buf.at[pl.ds(0, fed_rows)],
            send_sem=wrap_send,
            recv_sem=q_recv.at[0],
            device_id=at_place(me),
            device_id_type=MESH,
        ).wait_send()

    all_num.wait_recv()
    all_tot.wait_recv()
    num = jnp.sum(num_in[...].astype(jnp.float32), axis=0)
    tot = jnp.sum(tot_in[...], axis=0)
    at = lax.broadcasted_iota(jnp.int32, (rows, LANES), 0) + lax.rem(me, devs) * rows
    tot = jnp.where(lax.broadcasted_iota(jnp.int32, (rows, LANES), 1) == at, tot, 0.0)
    o_ref[...] = (num / jnp.sum(tot, axis=1, keepdims=True)).astype(jnp.bfloat16)
    all_num.wait_send()
    all_tot.wait_send()


def body(queries, key_pages, value_pages, page_owner, page_local, seq_lengths):
    n = lax.axis_size("seq")
    per, all_heads, head_dim = queries.shape
    pool, kv, page, _ = key_pages.shape
    heads = all_heads // lax.axis_size("tp")
    rows = per * heads
    seqs, slots = page_owner.shape
    devs = PHASE_ROWS // rows
    assert kv == 1 and pool == LANES and head_dim == LANES and seqs == n * per
    tokens = pool * page
    dma = pltpu.SemaphoreType.DMA
    out = pl.pallas_call(
        functools.partial(kernel, n),
        out_shape=pltpu.VMEM((rows, head_dim), jnp.bfloat16),
        in_specs=[pl.BlockSpec(memory_space=pl.ANY)] * 6,
        out_specs=pl.BlockSpec(memory_space=pltpu.VMEM),
        scratch_shapes=[
            pltpu.VMEM(queries.shape, jnp.bfloat16),
            pltpu.VMEM((tokens, head_dim), jnp.bfloat16),
            pltpu.VMEM((tokens, head_dim), jnp.bfloat16),
            pltpu.VMEM((seqs, slots), jnp.int32),
            pltpu.VMEM((seqs, slots), jnp.int32),
            pltpu.SMEM((seqs,), jnp.int32),
            pltpu.VMEM((n, rows, head_dim), jnp.bfloat16),
            pltpu.VMEM((HI, tokens // HI), jnp.float32),
            pltpu.VMEM((n, rows, head_dim), jnp.bfloat16),
            pltpu.VMEM((n // devs, 1, LANES), jnp.float32),
            pltpu.VMEM((n, rows, head_dim), jnp.bfloat16),
            pltpu.VMEM((n, 1, LANES), jnp.float32),
            dma((6,)),
            dma,
            dma,
            dma,
            dma,
            dma,
            dma((WRAP_PHASES,)),
            dma((n,)),
            dma,
            dma,
            dma,
            dma,
            pltpu.SemaphoreType.REGULAR,
            pltpu.SemaphoreType.REGULAR,
            pltpu.SemaphoreType.REGULAR,
            pltpu.SemaphoreType.REGULAR((WRAP,)),
        ],
        compiler_params=pltpu.CompilerParams(collective_id=0, has_side_effects=True),
        name="paged_attention",
    )(
        queries,
        key_pages.reshape(tokens, head_dim),
        value_pages.reshape(tokens, head_dim),
        page_owner,
        page_local,
        seq_lengths,
    )
    return out.reshape(per, heads, head_dim)


def solution(mesh):
    placed = (
        P(("rep", "seq"), None, None),
        P(("rep", "seq"), "tp", None, None),
        P(("rep", "seq"), "tp", None, None),
        P("rep", None),
        P("rep", None),
        P("rep"),
    )
    return jax.shard_map(
        body, mesh=mesh, in_specs=placed, out_specs=P(("rep", "seq"), "tp", None), check_vma=False
    )
```
